8 devices in a mesh: dp: 1 (over z), y: 2 (over y), x: 4 (over x, core).
Axes of the slice: x: 2, y: 2, z: 1, core: 2. Of those that a mesh axis runs over, the one named last changes fastest.
Arguments:
- tokens: int32 [3, 128], P(None, 'dp')
- lengths: int32 [128], P('dp')
- choices: int32 [3, 128, 2], P(None, 'dp')
- emb_table: bfloat16 [122753, 2304], P(None, 'x')
- k_cache: bfloat16 [128, 128, 36, 64], P('dp', None, 'y')
- v_cache: bfloat16 [128, 128, 36, 64], P('dp', None, 'y')
- g_attn: bfloat16 [2304], P('x')
- w_q: bfloat16 [2304, 2304], P('x', 'y')
- w_k: bfloat16 [2304, 2304], P('x', 'y')
- w_v: bfloat16 [2304, 2304], P('x', 'y')
- w_o: bfloat16 [2304, 2304], P('y', 'x')
- g_ffn: bfloat16 [2304], P('x')
- w_router: bfloat16 [2304, 8], P('x')
- w_act: bfloat16 [8, 2304, 5760], P(None, 'x', 'y')
- w_lin: bfloat16 [8, 2304, 5760], P(None, 'x', 'y')
- w_down: bfloat16 [8, 5760, 2304], P(None, 'y', 'x')
Outputs:
- output 1: bfloat16 [3, 128, 2304], P(None, 'dp', 'x')
- output 2: bfloat16 [128, 128, 36, 64], P('dp', None, 'y')
- output 3: bfloat16 [128, 128, 36, 64], P('dp', None, 'y')
All inputs are finite; a program needn't handle non-finite values.
Results may differ from the reference program's by a relative error of at most 0.012595.
Values are sent between devices in bfloat16 or wider.
A program may use at most 1.5 GiB of HBM per device.

```python
import math
import jax
import jax.numpy as jnp
from jax import lax

BATCH = 128
SEQ = 128
D = 2304
HEADS = 36
KV_HEADS = 36
HEAD = 64
FF = 5760
EXPERTS = 8
TOP = 2
VOCAB = 122753
STEPS = 3

EPS = 1e-5
ROPE_BASE = 1.0e6
LOG_SEQ = int(math.log2(SEQ))
HOT_COUNT = max(1, EXPERTS // 8)
GROUP_SIZE = HEADS // KV_HEADS


def draw_lengths(key_a, key_b, key_c):
    exponent = jax.random.randint(key_a, (BATCH,), 0, LOG_SEQ + 1)
    len_limit = jnp.minimum(jnp.left_shift(jnp.ones((BATCH,), jnp.int32), exponent), SEQ - 3)
    raw_draw = jax.random.randint(key_b, (BATCH,), 0, 1 << 30)
    lengths = 1 + raw_draw % len_limit
    pick_row = jax.random.randint(key_c, (), 0, BATCH)
    row_ids = jnp.arange(BATCH)
    lengths = jnp.where(row_ids == pick_row, SEQ - 3, lengths)
    lengths = jnp.where(row_ids == (pick_row + 1) % BATCH, 1, lengths)
    return lengths.astype(jnp.int32)


def draw_choices(key_a, key_b):
    expert_rank = jax.random.permutation(key_a, EXPERTS)
    hot_bonus = jnp.where(expert_rank < HOT_COUNT, EXPERTS, 0)
    noise_int = jax.random.randint(key_b, (STEPS, BATCH, EXPERTS), 0, 2 * EXPERTS)
    scores = (noise_int + hot_bonus) * EXPERTS + jnp.arange(EXPERTS)
    return lax.top_k(scores, TOP)[1].astype(jnp.int32)


def normal_weights(key_w, shape_w, scale_w):
    return (jax.random.normal(key_w, shape_w, jnp.float32) * scale_w).astype(jnp.bfloat16)


def setup_inputs(seed: int = 0, part: int = 0) -> dict:
    base_key = jax.random.key(seed)
    weight_keys = jax.random.split(base_key, 12)
    part_keys = jax.random.split(jax.random.fold_in(base_key, part), 8)
    tokens = jax.random.randint(part_keys[0], (STEPS, BATCH), 0, VOCAB)
    lengths = draw_lengths(part_keys[1], part_keys[2], part_keys[3])
    choices = draw_choices(part_keys[4], part_keys[5])
    k_cache = normal_weights(part_keys[6], (BATCH, SEQ, KV_HEADS, HEAD), 1.0)
    v_cache = normal_weights(part_keys[7], (BATCH, SEQ, KV_HEADS, HEAD), 1.0)
    ramp_rate = jax.random.uniform(weight_keys[0], (), jnp.float32, 0.6, 1.2)
    col_scale = jnp.exp(ramp_rate * jnp.linspace(-1.0, 1.0, D))
    emb_table = (jax.random.normal(weight_keys[1], (VOCAB, D), jnp.float32) * col_scale).astype(jnp.bfloat16)
    g_attn = (1.0 + 0.3 * jax.random.normal(weight_keys[2], (D,), jnp.float32)).astype(jnp.bfloat16)
    w_q = normal_weights(weight_keys[3], (D, HEADS * HEAD), D ** -0.5)
    w_k = normal_weights(weight_keys[4], (D, KV_HEADS * HEAD), D ** -0.5)
    w_v = normal_weights(weight_keys[5], (D, KV_HEADS * HEAD), D ** -0.5)
    w_o = normal_weights(weight_keys[6], (HEADS * HEAD, D), (HEADS * HEAD) ** -0.5)
    g_ffn = (1.0 + 0.3 * jax.random.normal(weight_keys[7], (D,), jnp.float32)).astype(jnp.bfloat16)
    w_router = normal_weights(weight_keys[8], (D, EXPERTS), 1.5 * D ** -0.5)
    w_act = normal_weights(weight_keys[9], (EXPERTS, D, FF), D ** -0.5)
    w_lin = normal_weights(weight_keys[10], (EXPERTS, D, FF), D ** -0.5)
    w_down = normal_weights(weight_keys[11], (EXPERTS, FF, D), FF ** -0.5)
    return dict(tokens=tokens, lengths=lengths, choices=choices, emb_table=emb_table, k_cache=k_cache, v_cache=v_cache, g_attn=g_attn, w_q=w_q, w_k=w_k, w_v=w_v, w_o=w_o, g_ffn=g_ffn, w_router=w_router, w_act=w_act, w_lin=w_lin, w_down=w_down)


def rms_norm(x_val, gain_vec):
    x_f32 = x_val.astype(jnp.float32)
    meansq = jnp.sum(x_f32 * x_f32, axis=-1, keepdims=True) / D
    return (x_f32 * lax.rsqrt(meansq + EPS) * gain_vec.astype(jnp.float32)).astype(jnp.bfloat16)


def rotate(vectors, positions):
    half_dim = HEAD // 2
    inv_freq = ROPE_BASE ** (-(jnp.arange(half_dim).astype(jnp.float32) * 2.0 / HEAD))
    angles = positions.astype(jnp.float32)[:, None, None] * inv_freq
    cosine = jnp.cos(angles)
    sine_val = jnp.sin(angles)
    first_half = vectors[..., :half_dim].astype(jnp.float32)
    second_half = vectors[..., half_dim:].astype(jnp.float32)
    return jnp.concatenate([first_half * cosine - second_half * sine_val, second_half * cosine + first_half * sine_val], axis=-1).astype(jnp.bfloat16)


def attend_row(row_args):
    q_row, key_row, val_row, pos_row = row_args
    scores = jnp.einsum('kgh,skh->kgs', q_row.astype(jnp.float32), key_row.astype(jnp.float32)) * HEAD ** -0.5
    valid_mask = jnp.arange(SEQ) <= pos_row
    scores = jnp.where(valid_mask, scores, -1.0e30)
    peak_val = jnp.max(scores, axis=-1, keepdims=True)
    weight = jnp.where(valid_mask, jnp.exp(scores - peak_val), 0.0)
    total_w = jnp.sum(weight, axis=-1, keepdims=True)
    mixed_out = jnp.einsum('kgs,skh->kgh', weight.astype(jnp.bfloat16).astype(jnp.float32), val_row.astype(jnp.float32))
    return (mixed_out / total_w).astype(jnp.bfloat16)


def reference(tokens, lengths, choices, emb_table, k_cache, v_cache, g_attn, w_q, w_k, w_v, w_o, g_ffn, w_router, w_act, w_lin, w_down):
    slot_ids = jnp.arange(SEQ)
    expert_ids = jnp.arange(EXPERTS)

    def one_step(carry, step_in):
        key_cache, val_cache = carry
        tok_row, choice_row, step_idx = step_in
        positions = lengths + step_idx
        x_in = emb_table[tok_row]
        normed = rms_norm(x_in, g_attn)
        queries = rotate(jnp.dot(normed, w_q, preferred_element_type=jnp.float32).astype(jnp.bfloat16).reshape(BATCH, HEADS, HEAD), positions)
        new_keys = rotate(jnp.dot(normed, w_k, preferred_element_type=jnp.float32).astype(jnp.bfloat16).reshape(BATCH, KV_HEADS, HEAD), positions)
        new_vals = jnp.dot(normed, w_v, preferred_element_type=jnp.float32).astype(jnp.bfloat16).reshape(BATCH, KV_HEADS, HEAD)
        hit_mask = (slot_ids[None, :] == positions[:, None])[:, :, None, None]
        key_cache = jnp.where(hit_mask, new_keys[:, None], key_cache)
        val_cache = jnp.where(hit_mask, new_vals[:, None], val_cache)
        grouped = queries.reshape(BATCH, KV_HEADS, GROUP_SIZE, HEAD)
        mixed = lax.map(attend_row, (grouped, key_cache, val_cache, positions)).reshape(BATCH, HEADS * HEAD)
        x_mid = (x_in.astype(jnp.float32) + jnp.dot(mixed, w_o, preferred_element_type=jnp.float32)).astype(jnp.bfloat16)
        normed2 = rms_norm(x_mid, g_ffn)
        logits = jnp.dot(normed2, w_router, preferred_element_type=jnp.float32)
        gate_val = jax.nn.softmax(jnp.take_along_axis(logits, choice_row, axis=1), axis=-1)
        onehot = choice_row[:, :, None] == expert_ids[None, None, :]
        coef = jnp.sum(jnp.where(onehot, gate_val[:, :, None], 0.0), axis=1)

        def expert_out(expert_args):
            act_w, lin_w, down_w, coef_col = expert_args
            act_f32 = jnp.dot(normed2, act_w, preferred_element_type=jnp.float32)
            lin_f32 = jnp.dot(normed2, lin_w, preferred_element_type=jnp.float32)
            unit_bf16 = (coef_col[:, None] * jax.nn.silu(act_f32) * lin_f32).astype(jnp.bfloat16)
            return jnp.dot(unit_bf16, down_w, preferred_element_type=jnp.float32)

        moe_sum = jnp.sum(lax.map(expert_out, (w_act, w_lin, w_down, coef.T)), axis=0)
        hidden_out = (x_mid.astype(jnp.float32) + moe_sum).astype(jnp.bfloat16)
        return (key_cache, val_cache), hidden_out

    (k_out, v_out), hidden_out = lax.scan(one_step, (k_cache, v_cache), (tokens, choices, jnp.arange(STEPS)))
    return hidden_out, k_out, v_out
```

```python
import functools
import jax
import jax.numpy as jnp
from jax import lax
from jax.experimental import pallas as pl
from jax.experimental.pallas import tpu as pltpu
from jax.sharding import PartitionSpec as P

EPS = 1e-5
ROPE_BASE = 1.0e6
LANES = 128
GROUP = 8
SLOTS = 4
TILE = 128
VMEM_BYTES = 60 * 1024 * 1024
CORE_PERM = [(0, 1), (1, 0), (2, 3), (3, 2)]
CHIP_PERM = [(0, 2), (2, 0), (1, 3), (3, 1)]
F32 = jnp.float32
BF16 = jnp.bfloat16


def params(**kw):
    return pltpu.CompilerParams(vmem_limit_bytes=VMEM_BYTES, **kw)


def gather_rows(tokens, emb_table):
    n_tok = tokens.shape[0]
    vocab, width = emb_table.shape
    last_tile = vocab // LANES - 1
    tail_at = (last_tile + 1) * LANES
    n_tail = vocab - tail_at
    n_groups = n_tok // GROUP
    per_chunk = LANES // GROUP

    def kernel(tok_s, tokv_ref, tail_ref, emb_ref, out_ref, sq_ref, buf, acc, sems):
        def copy(g, i):
            tile = jnp.minimum(tok_s[g * GROUP + i] // LANES, last_tile)
            slot = lax.rem(g, SLOTS)
            return pltpu.make_async_copy(
                emb_ref.at[:, pl.ds(pl.multiple_of(tile * LANES, LANES), LANES)],
                buf.at[slot, :, pl.ds(i * LANES, LANES)], sems.at[slot, i])

        def start(g):
            for i in range(GROUP):
                copy(g, i).start()

        for g in range(SLOTS - 1):
            start(g)
        lane_id = lax.broadcasted_iota(jnp.int32, (LANES, LANES), 0)
        col_id = lax.broadcasted_iota(jnp.int32, (LANES, LANES), 1)

        def step(g, carry):
            @pl.when(g + SLOTS - 1 < n_groups)
            def _():
                start(g + SLOTS - 1)
            for i in range(GROUP):
                copy(g, i).wait()
            slot = lax.rem(g, SLOTS)
            chunk = g // per_chunk
            base = lax.rem(g, per_chunk) * GROUP
            picks = []
            for i in range(GROUP):
                tok = tok_s[g * GROUP + i]
                lane = jnp.where(tok < tail_at, lax.rem(tok, LANES), -1)
                picks.append(((lane_id == lane) & (col_id == base + i)).astype(F32).astype(BF16))
            part = jnp.dot(buf[slot], jnp.concatenate(picks, axis=0), preferred_element_type=F32)

            @pl.when(base == 0)
            def _():
                acc[chunk] = part

            @pl.when(base != 0)
            def _():
                acc[chunk] += part
            return carry

        lax.fori_loop(0, n_groups, step, 0)
        for c in range(n_tok // LANES):
            rows = jnp.transpose(acc[c])
            tok_col = tokv_ref[pl.ds(c * LANES, LANES), :]
            for k in range(n_tail):
                rows = jnp.where(tok_col == tail_at + k, tail_ref[pl.ds(k, 1), :].astype(F32), rows)
            out_ref[pl.ds(c * LANES, LANES), :] = rows.astype(BF16)
            sq_ref[pl.ds(c * LANES, LANES), :] = jnp.sum(rows * rows, axis=1, keepdims=True)

    return pl.pallas_call(
        kernel,
        out_shape=(jax.ShapeDtypeStruct((n_tok, width), BF16), jax.ShapeDtypeStruct((n_tok, 1), F32)),
        grid_spec=pltpu.PrefetchScalarGridSpec(
            num_scalar_prefetch=1, grid=(),
            in_specs=[pl.BlockSpec(memory_space=pltpu.VMEM), pl.BlockSpec(memory_space=pltpu.VMEM), pl.BlockSpec(memory_space=pl.ANY)],
            out_specs=[pl.BlockSpec(memory_space=pltpu.VMEM)] * 2,
            scratch_shapes=[pltpu.VMEM((SLOTS, width, GROUP * LANES), BF16), pltpu.VMEM((n_tok // LANES, width, LANES), F32), pltpu.SemaphoreType.DMA((SLOTS, GROUP))]),
        compiler_params=params(),
        cost_estimate=pl.CostEstimate(flops=2 * n_tok * width * LANES * LANES, bytes_accessed=n_tok * width * LANES * 2, transcendentals=0),
        name="gather_rows",
    )(tokens, tokens[:, None], emb_table[tail_at:], emb_table.T)


def put_columns(block, columns, pick, hit):
    new = jnp.dot(columns, pick, preferred_element_type=F32)
    return jnp.where(hit, new.astype(BF16), block)


def column_scratch(rows_ref, out_ref):
    rows = rows_ref[...].astype(F32)
    pad = jnp.zeros((LANES - rows.shape[0], rows.shape[1]), F32)
    out_ref[...] = jnp.transpose(jnp.concatenate([rows, pad], axis=0)).astype(BF16)


def slot_masks(pos, row_local, per_q, steps, shape):
    col = lax.broadcasted_iota(jnp.int32, (LANES, shape[1]), 0)
    slot = lax.broadcasted_iota(jnp.int32, (LANES, shape[1]), 1)
    t = col // per_q
    pick = ((lax.rem(col, per_q) == row_local) & (slot == pos + t) & (t < steps)).astype(F32).astype(BF16)
    lane = lax.broadcasted_iota(jnp.int32, shape, 1)
    hit = (lane >= pos) & (lane < pos + steps)
    return pick, hit


def attend_quarter(quarter, lengths, q_rows, k_rows, v_rows, k_cache, v_cache, heads, steps):
    batch, kv_width, slots = k_cache.shape
    per_q = q_rows.shape[0] // steps
    head = kv_width // heads
    h_pad = (heads + 7) // 8 * 8
    step_b = 4
    n_grid = per_q // step_b

    def kernel(qi, len_s, q_ref, kr_ref, vr_ref, kc_ref, vc_ref, o_ref, ko_ref, vo_ref, k_cols, v_cols):
        g = pl.program_id(0)

        @pl.when(g == 0)
        def _():
            column_scratch(kr_ref, k_cols)
            column_scratch(vr_ref, v_cols)
        row_h = lax.broadcasted_iota(jnp.int32, (h_pad, kv_width), 0)
        col_h = lax.broadcasted_iota(jnp.int32, (h_pad, kv_width), 1) // head
        diag = row_h == col_h
        srow_t = lax.broadcasted_iota(jnp.int32, (steps * h_pad, slots), 0) // h_pad
        scol = lax.broadcasted_iota(jnp.int32, (steps * h_pad, slots), 1)
        for i in range(step_b):
            bl = g * step_b + i
            pos = len_s[qi[0] * per_q + bl]
            pick, hit = slot_masks(pos, bl, per_q, steps, (kv_width, slots))
            keys = put_columns(kc_ref[i], k_cols[...], pick, hit)
            vals = put_columns(vc_ref[i], v_cols[...], pick, hit)
            ko_ref[i] = keys
            vo_ref[i] = vals
            wide = jnp.concatenate([jnp.where(diag, q_ref[pl.ds(t * per_q + bl, 1), :], 0.0) for t in range(steps)], axis=0).astype(BF16)
            s = jnp.dot(wide, keys, preferred_element_type=F32) * head ** -0.5
            ok = scol <= pos + srow_t
            s = jnp.where(ok, s, -1.0e30)
            e = jnp.where(ok, jnp.exp(s - jnp.max(s, axis=1, keepdims=True)), 0.0)
            total = jnp.sum(e, axis=1, keepdims=True)
            mix = lax.dot_general(e.astype(BF16), vals, (((1,), (1,)), ((), ())), preferred_element_type=F32) / total
            for t in range(steps):
                piece = jnp.where(diag, mix[t * h_pad:(t + 1) * h_pad], 0.0)
                o_ref[pl.ds(t * per_q + bl, 1), :] = jnp.sum(piece, axis=0, keepdims=True)

    cache_in = pl.BlockSpec((step_b, kv_width, slots), lambda g, qi, ln: (qi[0] * n_grid + g, 0, 0))
    whole = lambda a: pl.BlockSpec(a.shape, lambda g, qi, ln: (0, 0))
    return pl.pallas_call(
        kernel,
        out_shape=(jax.ShapeDtypeStruct(q_rows.shape, F32), jax.ShapeDtypeStruct(k_cache.shape, BF16), jax.ShapeDtypeStruct(v_cache.shape, BF16)),
        grid_spec=pltpu.PrefetchScalarGridSpec(
            num_scalar_prefetch=2, grid=(n_grid,),
            in_specs=[whole(q_rows), whole(k_rows), whole(v_rows), cache_in, cache_in],
            out_specs=[pl.BlockSpec(q_rows.shape, lambda g, qi, ln: (0, 0)), cache_in, cache_in],
            scratch_shapes=[pltpu.VMEM((kv_width, LANES), BF16)] * 2),
        compiler_params=params(),
        cost_estimate=pl.CostEstimate(flops=4 * per_q * kv_width * LANES * LANES, bytes_accessed=8 * per_q * kv_width * slots, transcendentals=0),
        name="attend_quarter",
    )(quarter, lengths, q_rows, k_rows, v_rows, k_cache, v_cache)


def copy_quarter(quarter, lengths, k_rows, v_rows, k_cache, v_cache, k_out, v_out, steps):
    batch, kv_width, slots = k_cache.shape
    per_q = k_rows.shape[0] // steps
    step_b = 4
    n_grid = per_q // step_b

    def kernel(qi, len_s, kr_ref, vr_ref, kc_ref, vc_ref, ka_ref, va_ref, ko_ref, vo_ref, k_cols, v_cols):
        g = pl.program_id(0)

        @pl.when(g == 0)
        def _():
            column_scratch(kr_ref, k_cols)
            column_scratch(vr_ref, v_cols)
        for i in range(step_b):
            bl = g * step_b + i
            pos = len_s[qi[0] * per_q + bl]
            pick, hit = slot_masks(pos, bl, per_q, steps, (kv_width, slots))
            ko_ref[i] = put_columns(kc_ref[i], k_cols[...], pick, hit)
            vo_ref[i] = put_columns(vc_ref[i], v_cols[...], pick, hit)

    cache_in = pl.BlockSpec((step_b, kv_width, slots), lambda g, qi, ln: (qi[0] * n_grid + g, 0, 0))
    whole = lambda a: pl.BlockSpec(a.shape, lambda g, qi, ln: (0, 0))
    anyspec = pl.BlockSpec(memory_space=pl.ANY)
    return pl.pallas_call(
        kernel,
        out_shape=(jax.ShapeDtypeStruct(k_cache.shape, BF16), jax.ShapeDtypeStruct(v_cache.shape, BF16)),
        grid_spec=pltpu.PrefetchScalarGridSpec(
            num_scalar_prefetch=2, grid=(n_grid,),
            in_specs=[whole(k_rows), whole(v_rows), cache_in, cache_in, anyspec, anyspec],
            out_specs=[cache_in, cache_in],
            scratch_shapes=[pltpu.VMEM((kv_width, LANES), BF16)] * 2),
        input_output_aliases={6: 0, 7: 1},
        compiler_params=params(),
        cost_estimate=pl.CostEstimate(flops=4 * per_q * kv_width * LANES * LANES, bytes_accessed=8 * per_q * kv_width * slots, transcendentals=0),
        name="copy_quarter",
    )(quarter, lengths, k_rows, v_rows, k_cache, v_cache, k_out, v_out)


def expert_tiles(off_s, e, body):
    lo, hi = off_s[e], off_s[e + 1]
    first = lo // 16 * 16
    n_tiles = jnp.where(hi > lo, (hi - first + TILE - 1) // TILE, 0)

    def step(i, carry):
        at = pl.multiple_of(first + i * TILE, 16)
        row = at + lax.broadcasted_iota(jnp.int32, (TILE, 1), 0)
        body(pl.ds(at, TILE), (row >= lo) & (row < hi))
        return carry
    lax.fori_loop(0, n_tiles, step, 0)


def up_experts(offsets, rows, w_act, w_lin, chunk, size, block):
    n_rows, depth = rows.shape
    experts = w_act.shape[0]

    def kernel(off_s, x_ref, a_ref, l_ref, out_ref):
        e = pl.program_id(0)

        def body(ds, mine):
            x = x_ref[ds, :]
            for k, w_ref in enumerate((a_ref, l_ref)):
                y = jnp.dot(x, w_ref[0, :, :size], preferred_element_type=F32)
                out_ref[k, ds, :] = jnp.where(mine, y.astype(BF16), out_ref[k, ds, :])
        expert_tiles(off_s, e, body)

    w_spec = pl.BlockSpec((1, depth, block), lambda e, off: (e, 0, chunk))
    return pl.pallas_call(
        kernel,
        out_shape=jax.ShapeDtypeStruct((2, n_rows, size), BF16),
        grid_spec=pltpu.PrefetchScalarGridSpec(
            num_scalar_prefetch=1, grid=(experts,),
            in_specs=[pl.BlockSpec(rows.shape, lambda e, off: (0, 0)), w_spec, w_spec],
            out_specs=pl.BlockSpec((2, n_rows, size), lambda e, off: (0, 0, 0))),
        compiler_params=params(),
        cost_estimate=pl.CostEstimate(flops=8 * TILE * experts * depth * size, bytes_accessed=4 * experts * depth * size, transcendentals=0),
        name="up_experts",
    )(offsets, rows, w_act, w_lin)


def down_experts(offsets, units, w_down_t, pos_a, pos_b):
    n_rows, depth = units.shape
    experts, width, _ = w_down_t.shape
    n_tok = pos_a.shape[0]

    def kernel(off_s, u_ref, w_ref, pa_ref, pb_ref, out_ref, acc):
        e = pl.program_id(0)

        @pl.when(e == 0)
        def _():
            acc[...] = jnp.zeros_like(acc)

        def body(ds, mine):
            y = lax.dot_general(u_ref[ds, :], w_ref[0], (((1,), (1,)), ((), ())), preferred_element_type=F32)
            acc[ds, :] = jnp.where(mine, y, acc[ds, :])
        expert_tiles(off_s, e, body)

        @pl.when(e == experts - 1)
        def _():
            col = lax.broadcasted_iota(jnp.int32, (n_tok, n_rows), 1)
            pick = ((col == pa_ref[...]) | (col == pb_ref[...])).astype(F32).astype(BF16)
            y = acc[...]
            high = y.astype(BF16)
            low = (y - high.astype(F32)).astype(BF16)
            out_ref[...] = (jnp.dot(pick, high, preferred_element_type=F32) + jnp.dot(pick, low, preferred_element_type=F32)).astype(BF16)

    whole = lambda a: pl.BlockSpec(a.shape, lambda e, off: (0, 0))
    return pl.pallas_call(
        kernel,
        out_shape=jax.ShapeDtypeStruct((n_tok, width), BF16),
        grid_spec=pltpu.PrefetchScalarGridSpec(
            num_scalar_prefetch=1, grid=(experts,),
            in_specs=[whole(units), pl.BlockSpec((1, width, depth), lambda e, off: (e, 0, 0)), whole(pos_a), whole(pos_b)],
            out_specs=pl.BlockSpec((n_tok, width), lambda e, off: (0, 0)),
            scratch_shapes=[pltpu.VMEM((n_rows, width), F32)]),
        compiler_params=params(),
        cost_estimate=pl.CostEstimate(flops=4 * TILE * experts * depth * width, bytes_accessed=2 * experts * depth * width, transcendentals=0),
        name="down_experts",
    )(offsets, units, w_down_t, pos_a, pos_b)


def solution(mesh):
    x_count = mesh.shape['x']
    cache_spec = P('dp', None, 'y', None)
    in_specs = (P(None, 'dp'), P('dp'), P(None, 'dp', None), P(None, 'x'), cache_spec, cache_spec, P('x'), P('x', 'y'), P('x', 'y'), P('x', 'y'), P('y', 'x'), P('x'), P('x', None), P(None, 'x', 'y'), P(None, 'x', 'y'), P(None, 'y', 'x'))
    out_specs = (P(None, 'dp', 'x'), cache_spec, cache_spec)

    def over_core(v):
        return lax.ppermute(v, 'x', CORE_PERM)

    def over_chip(v):
        return lax.ppermute(v, 'x', CHIP_PERM)

    def per_device(tokens, lengths, choices, emb_table, k_cache, v_cache, g_attn, w_q, w_k, w_v, w_o, g_ffn, w_router, w_act, w_lin, w_down):
        steps, n_batch = tokens.shape
        heads, head = k_cache.shape[2], k_cache.shape[3]
        kv_width = heads * head
        width = emb_table.shape[1]
        width_full = width * x_count
        experts, _, ff = w_act.shape
        n_tok = steps * n_batch
        per_q = n_batch // x_count
        q_rows_n = steps * per_q
        xi = lax.axis_index('x')
        core = lax.rem(xi, 2)
        chip = xi // 2
        order = jnp.array([0, 2, 1, 3], jnp.int32)
        rel = lax.bitwise_xor(order, xi)
        back = order[lax.bitwise_xor(jnp.arange(x_count, dtype=jnp.int32), xi)]

        def to_rel(a):
            a = a.reshape((steps, x_count, per_q) + a.shape[2:])
            return jnp.moveaxis(a, 1, 0)[rel].reshape((n_tok,) + a.shape[3:])

        def norm(rows, sq, gain):
            sq_abs = sq.reshape(x_count, q_rows_n)[back]
            total = lax.psum(sq_abs, 'x')[rel].reshape(n_tok, 1)
            return (rows.astype(F32) * lax.rsqrt(total / width_full + EPS) * gain.astype(F32)).astype(BF16)

        tok_rel = to_rel(tokens)
        flat = choices.reshape(n_tok * 2)
        hot = (flat[:, None] == jnp.arange(experts)[None, :])
        lower = (lax.broadcasted_iota(jnp.int32, (2 * n_tok, 2 * n_tok), 0) > lax.broadcasted_iota(jnp.int32, (2 * n_tok, 2 * n_tok), 1)).astype(BF16)
        before = jnp.dot(lower, hot.astype(BF16), preferred_element_type=F32).astype(jnp.int32)
        counts = jnp.sum(hot.astype(jnp.int32), axis=0)
        first = jnp.sum(jnp.where(jnp.arange(experts)[:, None] > jnp.arange(experts)[None, :], counts[None, :], 0), axis=1)
        offsets = jnp.concatenate([first, jnp.full((1,), 2 * n_tok, jnp.int32)])
        place = jnp.sum(jnp.where(hot, before + first[None, :], 0), axis=1).reshape(steps, n_batch, 2)
        pos_a = to_rel(place[:, :, 0])
        pos_b = to_rel(place[:, :, 1])
        choice_a = to_rel(choices[:, :, 0])
        choice_b = to_rel(choices[:, :, 1])

        x_in, sq_in = gather_rows(tok_rel, emb_table)
        h = norm(x_in, sq_in, g_attn)
        part = jnp.concatenate([jnp.dot(h, w, preferred_element_type=F32) for w in (w_q, w_k, w_v)], axis=1).astype(BF16)
        half = n_tok // 2
        got = over_core(part[half:])
        part = (part[:half].astype(F32) + got.astype(F32)).astype(BF16)
        got = over_chip(part[q_rows_n:])
        proj = (part[:q_rows_n].astype(F32) + got.astype(F32)).astype(BF16).astype(F32)
        len_q = lax.dynamic_slice(lengths, (xi * per_q,), (per_q,))
        positions = (len_q[None, :] + jnp.arange(steps)[:, None]).reshape(q_rows_n).astype(F32)
        inv_freq = ROPE_BASE ** (-(jnp.arange(head // 2, dtype=F32) * 2.0 / head))
        angles = jnp.tile(positions[:, None] * inv_freq[None, :], (1, 2 * heads))
        cosine, sine = jnp.cos(angles), jnp.sin(angles)
        low_half = (jnp.arange(kv_width) % head < head // 2)[None, :]

        def rotate(v):
            other = jnp.where(low_half, -jnp.roll(v, -(head // 2), axis=1), jnp.roll(v, head // 2, axis=1))
            return (v * cosine + other * sine).astype(BF16)

        queries = rotate(proj[:, :kv_width]).astype(F32)
        kv_new = jnp.concatenate([rotate(proj[:, kv_width:2 * kv_width]), proj[:, 2 * kv_width:].astype(BF16)], axis=1)
        k_view = k_cache.transpose(0, 2, 3, 1).reshape(n_batch, kv_width, -1)
        v_view = v_cache.transpose(0, 2, 3, 1).reshape(n_batch, kv_width, -1)
        mixed, k_out, v_out = attend_quarter(xi[None], lengths, queries, kv_new[:, :kv_width], kv_new[:, kv_width:], k_view, v_view, heads, steps)
        mixed = mixed.astype(BF16)
        mixed2 = jnp.concatenate([mixed, over_chip(mixed)], axis=0)
        mixed4 = jnp.concatenate([mixed2, over_core(mixed2)], axis=0)
        attn = jnp.dot(mixed4, w_o, preferred_element_type=F32).astype(BF16)
        attn_sum = attn.astype(F32) + lax.ppermute(attn, 'y', [(0, 1), (1, 0)]).astype(F32)
        x_mid = (x_in.astype(F32) + attn_sum).astype(BF16)

        kv_pair = jnp.stack([kv_new, over_chip(kv_new)])
        kv_far = over_core(kv_pair)

        x_mid32 = x_mid.astype(F32)
        h2 = norm(x_mid, jnp.sum(x_mid32 * x_mid32, axis=1, keepdims=True), g_ffn)
        r_part = jnp.dot(h2, w_router, preferred_element_type=F32)
        logits = lax.psum(r_part.reshape(x_count, q_rows_n, experts)[back], 'x')[rel].reshape(n_tok, experts)
        eid = jnp.arange(experts)[None, :]
        pair = jnp.stack([jnp.sum(jnp.where(choice_a[:, None] == eid, logits, 0.0), axis=1), jnp.sum(jnp.where(choice_b[:, None] == eid, logits, 0.0), axis=1)], axis=1)
        gates = jax.nn.softmax(pair, axis=-1)
        n_pair = 2 * n_tok
        quarter = n_pair // x_count
        own_row = (xi * quarter + jnp.arange(quarter))[:, None]
        coef = jnp.sum(jnp.where(pos_a[None, :] == own_row, gates[None, :, 0], 0.0) + jnp.where(pos_b[None, :] == own_row, gates[None, :, 1], 0.0), axis=1, keepdims=True)
        n_rows = n_pair + TILE
        row_id = jnp.arange(n_rows)[:, None]
        sort_rows = ((pos_a[None, :] == row_id) | (pos_b[None, :] == row_id)).astype(BF16)
        sorted_h = jnp.dot(sort_rows, h2, preferred_element_type=F32).astype(BF16)

        block = 1536
        sizes = [block, ff - block]
        units = []
        for c, size in enumerate(sizes):
            first_part = up_experts(offsets, sorted_h, w_act, w_lin, c, size, block)[:, :n_pair].reshape(2, 2, 2, quarter, size)
            keep = lax.dynamic_index_in_dim(first_part, core, 2, keepdims=False)
            send = lax.dynamic_index_in_dim(first_part, 1 - core, 2, keepdims=False)
            summed = (keep.astype(F32) + over_core(send).astype(F32)).astype(BF16)
            keep = lax.dynamic_index_in_dim(summed, chip, 1, keepdims=False)
            send = lax.dynamic_index_in_dim(summed, 1 - chip, 1, keepdims=False)
            act, lin = (v for v in (keep.astype(F32) + over_chip(send).astype(F32)).astype(BF16).astype(F32))
            unit = (coef * jax.nn.silu(act) * lin).astype(BF16)
            both = lax.dynamic_update_index_in_dim(jnp.stack([over_chip(unit)] * 2), unit, chip, 0)
            far = over_core(both)
            units.append(jnp.where(core == 0, jnp.stack([both, far], axis=1), jnp.stack([far, both], axis=1)).reshape(n_pair, size))
        unit_all = jnp.pad(jnp.concatenate(units, axis=1), ((0, TILE), (0, 0)))

        for rows, idx in ((kv_pair[1], 2), (kv_far[0], 1), (kv_far[1], 3)):
            k_out, v_out = copy_quarter(lax.bitwise_xor(xi, idx)[None], lengths, rows[:, :kv_width], rows[:, kv_width:], k_view, v_view, k_out, v_out, steps)

        moe = down_experts(offsets, unit_all, w_down.transpose(0, 2, 1), pos_a[:, None], pos_b[:, None])
        moe_sum = moe.astype(F32) + lax.ppermute(moe, 'y', [(0, 1), (1, 0)]).astype(F32)
        out = (x_mid32 + moe_sum).astype(BF16)
        out = jnp.moveaxis(out.reshape(x_count, steps, per_q, width)[back], 0, 1).reshape(steps, n_batch, width)

        def to_cache(v):
            return v.reshape(n_batch, heads, head, -1).transpose(0, 3, 1, 2)
        return out, to_cache(k_out), to_cache(v_out)

    return jax.shard_map(per_device, mesh=mesh, in_specs=in_specs, out_specs=out_specs, check_vma=False)
```

```python
import jax
import jax.numpy as jnp
from jax import lax
from jax.experimental import pallas as pl
from jax.experimental.pallas import tpu as pltpu
from jax.sharding import PartitionSpec as P

EPS = 1e-5
ROPE_BASE = 1.0e6
LANES = 128
GROUP = 8
SLOTS = 4
TILE = 128
BLOCK = 256
ORDER = (0, 2, 1, 3)
VMEM_BYTES = 60 * 1024 * 1024
CORE_PERM = [(0, 1), (1, 0), (2, 3), (3, 2)]
CHIP_PERM = [(0, 2), (2, 0), (1, 3), (3, 1)]
F32 = jnp.float32
BF16 = jnp.bfloat16


def params(**kw):
    return pltpu.CompilerParams(vmem_limit_bytes=VMEM_BYTES, **kw)


def gather_rows(tokens, emb_table):
    n_tok = tokens.shape[0]
    vocab, width = emb_table.shape
    last_tile = vocab // LANES - 1
    tail_at = (last_tile + 1) * LANES
    n_tail = vocab - tail_at
    n_groups = n_tok // GROUP
    per_chunk = LANES // GROUP
    n_chunks = (n_tok + LANES - 1) // LANES

    def kernel(tok_s, tokv_ref, tail_ref, emb_ref, out_ref, sq_ref, buf, acc, sems):
        def copy(g, i):
            tile = jnp.minimum(tok_s[g * GROUP + i] // LANES, last_tile)
            slot = lax.rem(g, SLOTS)
            return pltpu.make_async_copy(
                emb_ref.at[:, pl.ds(pl.multiple_of(tile * LANES, LANES), LANES)],
                buf.at[slot, :, pl.ds(i * LANES, LANES)], sems.at[slot, i])

        def start(g):
            for i in range(GROUP):
                copy(g, i).start()

        for g in range(SLOTS - 1):
            start(g)
        lane_id = lax.broadcasted_iota(jnp.int32, (LANES, LANES), 0)
        col_id = lax.broadcasted_iota(jnp.int32, (LANES, LANES), 1)

        def step(g, carry):
            @pl.when(g + SLOTS - 1 < n_groups)
            def _():
                start(g + SLOTS - 1)

            for i in range(GROUP):
                copy(g, i).wait()
            slot = lax.rem(g, SLOTS)
            chunk = g // per_chunk
            base = lax.rem(g, per_chunk) * GROUP
            picks = []
            for i in range(GROUP):
                tok = tok_s[g * GROUP + i]
                lane = jnp.where(tok < tail_at, lax.rem(tok, LANES), -1)
                picks.append(((lane_id == lane) & (col_id == base + i)).astype(F32).astype(BF16))
            pick = jnp.concatenate(picks, axis=0)
            for m in range(2):
                ds = pl.ds(m * (width // 2), width // 2)
                part = jnp.dot(buf[slot, ds, :], pick, preferred_element_type=F32)
                acc[chunk, ds, :] = jnp.where(base == 0, part, acc[chunk, ds, :] + part)
            return carry

        lax.fori_loop(0, n_groups, step, 0)
        for c in range(n_chunks):
            size = min(LANES, n_tok - c * LANES)
            rows = jnp.transpose(acc[c])[:size]
            tok_col = tokv_ref[pl.ds(c * LANES, size), :]
            for k in range(n_tail):
                rows = jnp.where(tok_col == tail_at + k, tail_ref[pl.ds(k, 1), :].astype(F32), rows)
            out_ref[pl.ds(c * LANES, size), :] = rows.astype(BF16)
            sq_ref[pl.ds(c * LANES, size), :] = jnp.sum(rows * rows, axis=1, keepdims=True)

    return pl.pallas_call(
        kernel,
        out_shape=(jax.ShapeDtypeStruct((n_tok, width), BF16), jax.ShapeDtypeStruct((n_tok, 1), F32)),
        grid_spec=pltpu.PrefetchScalarGridSpec(
            num_scalar_prefetch=1, grid=(),
            in_specs=[pl.BlockSpec(memory_space=pltpu.VMEM), pl.BlockSpec(memory_space=pltpu.VMEM), pl.BlockSpec(memory_space=pl.ANY)],
            out_specs=[pl.BlockSpec(memory_space=pltpu.VMEM)] * 2,
            scratch_shapes=[pltpu.VMEM((SLOTS, width, GROUP * LANES), BF16), pltpu.VMEM((n_chunks, width, LANES), F32), pltpu.SemaphoreType.DMA((SLOTS, GROUP))]),
        compiler_params=params(),
        cost_estimate=pl.CostEstimate(flops=2 * n_tok * width * LANES * LANES, bytes_accessed=n_tok * width * LANES * 2, transcendentals=0),
        name="gather_rows",
    )(tokens, tokens[:, None], emb_table[tail_at:], emb_table.T)


def column_scratch(rows_ref, out_ref):
    rows = rows_ref[...].astype(F32)
    pad = jnp.zeros((LANES - rows.shape[0], rows.shape[1]), F32)
    out_ref[...] = jnp.transpose(jnp.concatenate([rows, pad], axis=0)).astype(BF16)


def slot_masks(pos, row_local, per_q, steps, slots):
    col = lax.broadcasted_iota(jnp.int32, (LANES, slots), 0)
    slot = lax.broadcasted_iota(jnp.int32, (LANES, slots), 1)
    t = col // per_q
    pick = ((lax.rem(col, per_q) == row_local) & (slot == pos + t) & (t < steps)).astype(F32).astype(BF16)
    lane = lax.broadcasted_iota(jnp.int32, (16, slots), 1)
    keep = ((lane < pos) | (lane >= pos + steps)).astype(F32).astype(BF16)
    return pick, keep[:1]


def put_pair(blocks, columns, picks, keeps):
    slots = blocks[0].shape[1]
    new = jnp.dot(columns, jnp.concatenate(picks, axis=1), preferred_element_type=F32).astype(BF16)
    return [b * k + new[:, i * slots:(i + 1) * slots] for i, (b, k) in enumerate(zip(blocks, keeps))]


def cache_specs(k_cache, n_grid, step_b, skip=0):
    _, kv_width, slots = k_cache.shape
    return pl.BlockSpec((step_b, kv_width, slots), lambda g, qi, ln: (qi[0] * n_grid + skip + g, 0, 0))


def attend_quarter(quarter, lengths, q_rows, k_rows, v_rows, k_cache, v_cache, heads, steps):
    _, kv_width, slots = k_cache.shape
    per_q = q_rows.shape[0] // steps
    head = kv_width // heads
    h_pad = (heads + 7) // 8 * 8
    step_b = 4
    n_grid = per_q // step_b

    def kernel(qi, len_s, q_ref, kr_ref, vr_ref, kc_ref, vc_ref, o_ref, ko_ref, vo_ref, k_cols, v_cols):
        g = pl.program_id(0)

        @pl.when(g == 0)
        def _():
            column_scratch(kr_ref, k_cols)
            column_scratch(vr_ref, v_cols)

        row_h = lax.broadcasted_iota(jnp.int32, (h_pad, kv_width), 0)
        col_h = lax.broadcasted_iota(jnp.int32, (h_pad, kv_width), 1) // head
        diag = row_h == col_h
        srow_t = lax.broadcasted_iota(jnp.int32, (steps * h_pad, slots), 0) // h_pad
        scol = lax.broadcasted_iota(jnp.int32, (steps * h_pad, slots), 1)
        bls = [g * step_b + i for i in range(step_b)]
        poss = [len_s[qi[0] * per_q + bl] for bl in bls]
        picks, keeps = zip(*[slot_masks(pos, bl, per_q, steps, slots) for pos, bl in zip(poss, bls)])
        for i in range(0, step_b, 2):
            for src, cols, dst in ((kc_ref, k_cols, ko_ref), (vc_ref, v_cols, vo_ref)):
                for j, blk in enumerate(put_pair([src[i], src[i + 1]], cols[...], picks[i:i + 2], keeps[i:i + 2])):
                    dst[i + j] = blk
        scores, oks = [], []
        for i, (pos, bl) in enumerate(zip(poss, bls)):
            wide = jnp.concatenate([jnp.where(diag, q_ref[pl.ds(t * per_q + bl, 1), :], 0.0) for t in range(steps)], axis=0).astype(BF16)
            scores.append(jnp.dot(wide, ko_ref[i], preferred_element_type=F32) * head ** -0.5)
            oks.append((scol <= pos + srow_t).astype(F32))
        ok = jnp.concatenate(oks, axis=0) > 0.5
        s = jnp.where(ok, jnp.concatenate(scores, axis=0), -1.0e30)
        e = jnp.where(ok, jnp.exp(s - jnp.max(s, axis=1, keepdims=True)), 0.0)
        scale = 1.0 / jnp.sum(e, axis=1, keepdims=True)
        e = e.astype(BF16)
        n_row = steps * h_pad
        for i, bl in enumerate(bls):
            mine = slice(i * n_row, (i + 1) * n_row)
            mix = lax.dot_general(e[mine], vo_ref[i], (((1,), (1,)), ((), ())), preferred_element_type=F32) * scale[mine]
            for t in range(steps):
                piece = jnp.where(diag, mix[t * h_pad:(t + 1) * h_pad], 0.0)
                o_ref[pl.ds(t * per_q + bl, 1), :] = jnp.sum(piece, axis=0, keepdims=True)

    cache_in = cache_specs(k_cache, n_grid, step_b)
    whole = lambda a: pl.BlockSpec(a.shape, lambda g, qi, ln: (0, 0))
    return pl.pallas_call(
        kernel,
        out_shape=(jax.ShapeDtypeStruct(q_rows.shape, F32), jax.ShapeDtypeStruct(k_cache.shape, BF16), jax.ShapeDtypeStruct(v_cache.shape, BF16)),
        grid_spec=pltpu.PrefetchScalarGridSpec(
            num_scalar_prefetch=2, grid=(n_grid,),
            in_specs=[whole(q_rows), whole(k_rows), whole(v_rows), cache_in, cache_in],
            out_specs=[pl.BlockSpec(q_rows.shape, lambda g, qi, ln: (0, 0)), cache_in, cache_in],
            scratch_shapes=[pltpu.VMEM((kv_width, LANES), BF16)] * 2),
        compiler_params=params(),
        cost_estimate=pl.CostEstimate(flops=4 * per_q * kv_width * LANES * LANES, bytes_accessed=8 * per_q * kv_width * slots, transcendentals=0),
        name="attend_quarter",
    )(quarter, lengths, q_rows, k_rows, v_rows, k_cache, v_cache)


def copy_part(quarter, lengths, k_rows, v_rows, k_cache, v_cache, k_out, v_out, steps, part, n_parts, step_b):
    _, kv_width, slots = k_cache.shape
    per_q = k_rows.shape[0] // steps
    n_all = per_q // step_b
    n_grid = n_all // n_parts
    skip = part * n_grid

    def kernel(qi, len_s, kr_ref, vr_ref, kc_ref, vc_ref, ka_ref, va_ref, ko_ref, vo_ref, k_cols, v_cols):
        g = pl.program_id(0)

        @pl.when(g == 0)
        def _():
            column_scratch(kr_ref, k_cols)
            column_scratch(vr_ref, v_cols)

        for i in range(0, step_b, 2):
            bls = [(g + skip) * step_b + i + j for j in range(2)]
            poss = [len_s[qi[0] * per_q + bl] for bl in bls]
            picks, keeps = zip(*[slot_masks(pos, bl, per_q, steps, slots) for pos, bl in zip(poss, bls)])
            for src, cols, dst in ((kc_ref, k_cols, ko_ref), (vc_ref, v_cols, vo_ref)):
                for j, blk in enumerate(put_pair([src[i], src[i + 1]], cols[...], picks, keeps)):
                    dst[i + j] = blk

    cache_in = cache_specs(k_cache, n_all, step_b, skip)
    whole = lambda a: pl.BlockSpec(a.shape, lambda g, qi, ln: (0, 0))
    anyspec = pl.BlockSpec(memory_space=pl.ANY)
    return pl.pallas_call(
        kernel,
        out_shape=(jax.ShapeDtypeStruct(k_cache.shape, BF16), jax.ShapeDtypeStruct(v_cache.shape, BF16)),
        grid_spec=pltpu.PrefetchScalarGridSpec(
            num_scalar_prefetch=2, grid=(n_grid,),
            in_specs=[whole(k_rows), whole(v_rows), cache_in, cache_in, anyspec, anyspec],
            out_specs=[cache_in, cache_in],
            scratch_shapes=[pltpu.VMEM((kv_width, LANES), BF16)] * 2),
        input_output_aliases={6: 0, 7: 1},
        compiler_params=params(),
        cost_estimate=pl.CostEstimate(flops=4 * per_q // n_parts * kv_width * LANES * LANES, bytes_accessed=12 * per_q // n_parts * kv_width * slots, transcendentals=0),
        name="copy_part",
    )(quarter, lengths, k_rows, v_rows, k_cache, v_cache, k_out, v_out)


def expert_tiles(off_s, e, n_rows, body):
    lo, hi = off_s[e], off_s[e + 1]
    first = lo // 16 * 16
    n_tiles = jnp.where(hi > lo, (hi - first + TILE - 1) // TILE, 0)

    def step(i, carry):
        start = first + i * TILE
        at = pl.multiple_of(jnp.minimum(start, n_rows - TILE), 16)
        row = at + lax.broadcasted_iota(jnp.int32, (TILE, 1), 0)
        body(pl.ds(at, TILE), (row >= jnp.maximum(lo, start)) & (row < hi))
        return carry

    lax.fori_loop(0, n_tiles, step, 0)


def weight_specs(parts, per_quarter, blocks, depth):
    def spec(i, b):
        return pl.BlockSpec((1, depth, BLOCK), lambda e, rel, off: (e, 0, rel[i] * per_quarter + b))

    return [spec(i, b) for i in range(parts) for b in blocks]


def up_experts(rel, offsets, rows, w_act, w_lin, blocks, per_quarter):
    n_rows, depth = rows.shape
    experts, _, ff = w_act.shape
    parts, nb = rel.shape[0], len(blocks)
    n_w = parts * nb

    def kernel(rel_s, off_s, x_ref, *refs):
        a_refs, l_refs, (keep_ref, send_ref) = refs[:n_w], refs[n_w:2 * n_w], refs[2 * n_w:]
        e = pl.program_id(0)
        lane = lax.broadcasted_iota(jnp.int32, (1, BLOCK), 1)

        def body(ds, mine):
            x = x_ref[ds, :]
            for i in range(parts):
                for n, b in enumerate(blocks):
                    ok = mine & (lane + (rel_s[i] * per_quarter + b) * BLOCK < ff)
                    for k, w_refs in enumerate((a_refs, l_refs)):
                        out_ref = (keep_ref if i < 2 else send_ref).at[i % 2, k]
                        cols = pl.ds(n * BLOCK, BLOCK)
                        y = jnp.dot(x, w_refs[i * nb + n][0], preferred_element_type=F32)
                        out_ref[ds, cols] = jnp.where(ok, y, out_ref[ds, cols].astype(F32)).astype(BF16)

        @pl.when(e == 0)
        def _():
            keep_ref[...] = jnp.zeros_like(keep_ref)
            send_ref[...] = jnp.zeros_like(send_ref)

        expert_tiles(off_s, e, n_rows, body)

    shape = (2, 2, n_rows, nb * BLOCK)
    out = pl.BlockSpec(shape, lambda e, rel, off: (0, 0, 0, 0))
    cols = n_w * BLOCK
    return pl.pallas_call(
        kernel,
        out_shape=(jax.ShapeDtypeStruct(shape, BF16),) * 2,
        grid_spec=pltpu.PrefetchScalarGridSpec(
            num_scalar_prefetch=2, grid=(experts,),
            in_specs=[pl.BlockSpec(rows.shape, lambda e, rel, off: (0, 0))] + weight_specs(parts, per_quarter, blocks, depth) * 2,
            out_specs=[out, out]),
        compiler_params=params(),
        cost_estimate=pl.CostEstimate(flops=8 * TILE * experts * depth * cols, bytes_accessed=6 * experts * depth * cols, transcendentals=0),
        name="up_experts",
    )(rel, offsets, rows, *[w_act] * n_w, *[w_lin] * n_w)


def down_experts(rel, offsets, own, near, far, w_down_t, before, pos_a, pos_b, blocks, per_quarter, last):
    n_rows = own.shape[0]
    experts, width, ff = w_down_t.shape
    n_tok = pos_a.shape[0]
    parts, nb = rel.shape[0], len(blocks)
    n_w = parts * nb
    edge = ff - (ff - 1) // BLOCK * BLOCK
    has_edge = per_quarter - 1 in blocks

    def kernel(rel_s, off_s, own_ref, near_ref, far_ref, *refs):
        w_refs, refs = refs[:n_w], refs[n_w:]
        if before is not None:
            before_ref, refs = refs[0], refs[1:]
        if last:
            pa_ref, pb_ref, out_ref, acc = refs
        else:
            acc, = refs
        e = pl.program_id(0)

        @pl.when(e == 0)
        def _():
            acc[...] = jnp.zeros_like(acc) if before is None else before_ref[...]

        def body(ds, mine):
            def run(edge_part):
                total = acc[ds, :]
                for i in range(parts):
                    for n, b in enumerate(blocks):
                        cut = edge if i == edge_part and b == per_quarter - 1 else BLOCK
                        cols = pl.ds(n * BLOCK, cut)
                        u = (own_ref[ds, cols], near_ref[ds, cols], far_ref[0, ds, cols], far_ref[1, ds, cols])[i]
                        w = w_refs[i * nb + n][0, :, :cut]
                        total = total + lax.dot_general(u, w, (((1,), (1,)), ((), ())), preferred_element_type=F32)
                acc[ds, :] = jnp.where(mine, total, acc[ds, :])

            if has_edge:
                for i in range(parts):
                    @pl.when(rel_s[i] == parts - 1)
                    def _(i=i):
                        run(i)
            else:
                run(None)

        expert_tiles(off_s, e, n_rows, body)

        if last:
            @pl.when(e == experts - 1)
            def _():
                col = lax.broadcasted_iota(jnp.int32, (n_tok, n_rows), 1)
                pick = ((col == pa_ref[...]) | (col == pb_ref[...])).astype(F32).astype(BF16)
                y = acc[...]
                high = y.astype(BF16)
                low = (y - high.astype(F32)).astype(BF16)
                out_ref[...] = (jnp.dot(pick, high, preferred_element_type=F32) + jnp.dot(pick, low, preferred_element_type=F32)).astype(BF16)

    whole = lambda a: pl.BlockSpec(a.shape, lambda e, rel, off: (0,) * a.ndim)
    extra = ([] if before is None else [before]) + ([pos_a, pos_b] if last else [])
    acc_shape = (n_rows, width)
    if last:
        out_shape, scratch = jax.ShapeDtypeStruct((n_tok, width), BF16), [pltpu.VMEM(acc_shape, F32)]
    else:
        out_shape, scratch = jax.ShapeDtypeStruct(acc_shape, F32), []
    cols = n_w * BLOCK
    return pl.pallas_call(
        kernel,
        out_shape=out_shape,
        grid_spec=pltpu.PrefetchScalarGridSpec(
            num_scalar_prefetch=2, grid=(experts,),
            in_specs=[whole(own), whole(near), whole(far)] + weight_specs(parts, per_quarter, blocks, width) + [whole(a) for a in extra],
            out_specs=pl.BlockSpec(out_shape.shape, lambda e, rel, off: (0, 0)),
            scratch_shapes=scratch),
        compiler_params=params(),
        cost_estimate=pl.CostEstimate(flops=4 * TILE * experts * cols * width, bytes_accessed=4 * experts * cols * width, transcendentals=0),
        name="down_experts",
    )(rel, offsets, own, near, far, *[w_down_t] * n_w, *extra)


def share_rows(rows, sums):
    n_x, n_y = 4, 2
    peers = [(d, e) for d in range(n_x) for e in range(n_y) if d or e]

    def kernel(rows_ref, sums_ref, rows_out, sums_out, send_sems, recv_sems):
        xi, yi = lax.axis_index('x'), lax.axis_index('y')

        def peer(d, e):
            return {'x': lax.bitwise_xor(xi, d), 'y': lax.bitwise_xor(yi, e)}

        barrier = pltpu.get_barrier_semaphore()
        for d, e in peers:
            pl.semaphore_signal(barrier, inc=1, device_id=peer(d, e), device_id_type=pl.DeviceIdType.MESH)
        pl.semaphore_wait(barrier, len(peers))
        copies = [pltpu.make_async_remote_copy(
            src_ref=rows_ref, dst_ref=rows_out.at[yi], send_sem=send_sems.at[0], recv_sem=recv_sems.at[0],
            device_id=peer(0, 1), device_id_type=pl.DeviceIdType.MESH)]
        copies += [pltpu.make_async_remote_copy(
            src_ref=sums_ref, dst_ref=sums_out.at[d, yi], send_sem=send_sems.at[k + 1], recv_sem=recv_sems.at[k + 1],
            device_id=peer(d, e), device_id_type=pl.DeviceIdType.MESH) for k, (d, e) in enumerate(peers)]
        for c in copies:
            c.start()
        rows_out[yi] = rows_ref[...]
        sums_out[0, yi] = sums_ref[...]
        for c in copies:
            c.wait()

    return pl.pallas_call(
        kernel,
        out_shape=(jax.ShapeDtypeStruct((n_y,) + rows.shape, rows.dtype), jax.ShapeDtypeStruct((n_x, n_y) + sums.shape, sums.dtype)),
        in_specs=[pl.BlockSpec(memory_space=pltpu.VMEM)] * 2,
        out_specs=[pl.BlockSpec(memory_space=pltpu.VMEM)] * 2,
        scratch_shapes=[pltpu.SemaphoreType.DMA((len(peers) + 1,))] * 2,
        compiler_params=pltpu.CompilerParams(collective_id=0, has_side_effects=True),
        cost_estimate=pl.CostEstimate(flops=0, bytes_accessed=16_000_000, transcendentals=0),
        name="share_rows",
    )(rows, sums)


def share_small(values, call_id):
    n_dev = 4

    def kernel(v_ref, out_ref, send_sems, recv_sems):
        xi = lax.axis_index('x')
        barrier = pltpu.get_barrier_semaphore()
        for d in range(1, n_dev):
            pl.semaphore_signal(barrier, inc=1, device_id={'x': lax.bitwise_xor(xi, d)}, device_id_type=pl.DeviceIdType.MESH)
        pl.semaphore_wait(barrier, n_dev - 1)
        copies = []
        for d in range(1, n_dev):
            copies.append(pltpu.make_async_remote_copy(
                src_ref=v_ref, dst_ref=out_ref.at[d], send_sem=send_sems.at[d - 1], recv_sem=recv_sems.at[d - 1],
                device_id={'x': lax.bitwise_xor(xi, d)}, device_id_type=pl.DeviceIdType.MESH))
            copies[-1].start()
        out_ref[0] = v_ref[...]
        for c in copies:
            c.wait()

    return pl.pallas_call(
        kernel,
        out_shape=jax.ShapeDtypeStruct((n_dev,) + values.shape, values.dtype),
        in_specs=[pl.BlockSpec(memory_space=pltpu.VMEM)],
        out_specs=pl.BlockSpec(memory_space=pltpu.VMEM),
        scratch_shapes=[pltpu.SemaphoreType.DMA((n_dev - 1,))] * 2,
        compiler_params=pltpu.CompilerParams(collective_id=call_id, has_side_effects=True),
        cost_estimate=pl.CostEstimate(flops=0, bytes_accessed=8_000_000, transcendentals=0),
        name="share_small",
    )(values)


def solution(mesh):
    x_count = mesh.shape['x']
    cache_spec = P('dp', None, 'y', None)
    in_specs = (P(None, 'dp'), P('dp'), P(None, 'dp', None), P(None, 'x'), cache_spec, cache_spec, P('x'), P('x', 'y'), P('x', 'y'), P('x', 'y'), P('y', 'x'), P('x'), P('x', None), P(None, 'x', 'y'), P(None, 'x', 'y'), P(None, 'y', 'x'))
    out_specs = (P(None, 'dp', 'x'), cache_spec, cache_spec)

    def over_core(v):
        return lax.ppermute(v, 'x', CORE_PERM)

    def over_chip(v):
        return lax.ppermute(v, 'x', CHIP_PERM)

    def layer_steps(tokens, lengths, choices, emb_table, k_cache, v_cache, g_attn, w_q, w_k, w_v, w_o, g_ffn, w_router, w_act, w_lin, w_down):
        steps, n_batch = tokens.shape
        heads, head = k_cache.shape[2], k_cache.shape[3]
        kv_width = heads * head
        width = emb_table.shape[1]
        width_full = width * x_count
        experts, _, ff = w_act.shape
        n_tok = steps * n_batch
        per_q = n_batch // x_count
        q_rows_n = steps * per_q
        xi = lax.axis_index('x')
        order = jnp.array(ORDER, jnp.int32)
        rel = lax.bitwise_xor(order, xi)
        back = order[lax.bitwise_xor(jnp.arange(x_count, dtype=jnp.int32), xi)]

        def to_rel(a):
            a = a.reshape((steps, x_count, per_q) + a.shape[2:])
            return jnp.moveaxis(a, 1, 0)[rel].reshape((n_tok,) + a.shape[3:])

        def shared(v, call_id):
            r = v.shape[0]
            v = jnp.pad(v, ((0, -r % 8), (0, 0)))
            got = share_small(jnp.moveaxis(v.reshape(-1, x_count, q_rows_n), 1, 0), call_id)
            rows = [[got[d, ORDER[ORDER[i] ^ d], :r] for i in range(x_count)] for d in range(x_count)]
            return jnp.stack([jnp.concatenate(one, axis=1) for one in rows])

        yi = lax.axis_index('y')
        y_rows = n_tok // 2
        my_tokens = lax.dynamic_slice(to_rel(tokens), (yi * y_rows,), (y_rows,))
        my_rows, my_sq = gather_rows(my_tokens, emb_table)
        both_rows, each_sq = share_rows(my_rows, jnp.pad(my_sq.reshape(2, 1, q_rows_n), ((0, 0), (0, 7), (0, 0))))
        x_in = both_rows.reshape(n_tok, width)
        found = [[ORDER[ORDER[i] ^ d] for d in range(x_count)] for i in range(x_count)]
        total_sq = jnp.stack([sum(each_sq[d, j // 2, j % 2, 0] for d, j in enumerate(js)) for js in found]).reshape(n_tok, 1)
        h = (x_in.astype(F32) * lax.rsqrt(total_sq / width_full + EPS) * g_attn.astype(F32)).astype(BF16)
        part = jnp.concatenate([jnp.dot(h, w, preferred_element_type=F32) for w in (w_q, w_k, w_v)], axis=1).astype(BF16)

        choices, lengths_r, part = lax.optimization_barrier((choices, lengths, part))
        flat = choices.reshape(n_tok * 2)
        hot = (flat[:, None] == jnp.arange(experts)[None, :])
        lower = (lax.broadcasted_iota(jnp.int32, (2 * n_tok, 2 * n_tok), 0) > lax.broadcasted_iota(jnp.int32, (2 * n_tok, 2 * n_tok), 1)).astype(BF16)
        before = jnp.dot(lower, hot.astype(BF16), preferred_element_type=F32).astype(jnp.int32)
        counts = jnp.sum(hot.astype(jnp.int32), axis=0)
        first = jnp.sum(jnp.where(jnp.arange(experts)[:, None] > jnp.arange(experts)[None, :], counts[None, :], 0), axis=1)
        offsets = jnp.concatenate([first, jnp.full((1,), 2 * n_tok, jnp.int32)])
        place = jnp.sum(jnp.where(hot, before + first[None, :], 0), axis=1).reshape(steps, n_batch, 2)
        pos_a = to_rel(place[:, :, 0])
        pos_b = to_rel(place[:, :, 1])
        choice_a = to_rel(choices[:, :, 0])
        choice_b = to_rel(choices[:, :, 1])

        half = n_tok // 2
        got = over_core(part[half:])
        part = (part[:half].astype(F32) + got.astype(F32)).astype(BF16)
        got = over_chip(part[q_rows_n:])
        proj = (part[:q_rows_n].astype(F32) + got.astype(F32)).astype(BF16).astype(F32)
        len_q = lax.dynamic_slice(lengths_r, (xi * per_q,), (per_q,))
        positions = (len_q[None, :] + jnp.arange(steps)[:, None]).reshape(q_rows_n).astype(F32)
        inv_freq = ROPE_BASE ** (-(jnp.arange(head // 2, dtype=F32) * 2.0 / head))
        angles = jnp.tile(positions[:, None] * inv_freq[None, :], (1, 2 * heads))
        cosine, sine = jnp.cos(angles), jnp.sin(angles)
        low_half = (jnp.arange(kv_width) % head < head // 2)[None, :]

        def rotate(v):
            other = jnp.where(low_half, -jnp.roll(v, -(head // 2), axis=1), jnp.roll(v, head // 2, axis=1))
            return (v * cosine + other * sine).astype(BF16)

        queries = rotate(proj[:, :kv_width]).astype(F32)
        kv_new = jnp.concatenate([rotate(proj[:, kv_width:2 * kv_width]), proj[:, 2 * kv_width:].astype(BF16)], axis=1)
        k_view = k_cache.transpose(0, 2, 3, 1).reshape(n_batch, kv_width, -1)
        v_view = v_cache.transpose(0, 2, 3, 1).reshape(n_batch, kv_width, -1)
        mixed, k_out, v_out = attend_quarter(xi[None], lengths, queries, kv_new[:, :kv_width], kv_new[:, kv_width:], k_view, v_view, heads, steps)
        mixed = mixed.astype(BF16)
        mixed2 = jnp.concatenate([mixed, over_chip(mixed)], axis=0)
        mixed4 = jnp.concatenate([mixed2, over_core(mixed2)], axis=0)
        attn = jnp.dot(mixed4, w_o, preferred_element_type=F32).astype(BF16)

        kv_pair = jnp.stack([kv_new, over_chip(kv_new)])
        kv_far = over_core(kv_pair)

        def write(caches, rows, idx, part, n_parts, step_b):
            return copy_part(lax.bitwise_xor(xi, idx)[None], lengths, rows[:, :kv_width], rows[:, kv_width:], k_view, v_view, *caches, steps, part, n_parts, step_b)

        def add_over_y(v):
            got = lax.ppermute(v, 'y', [(0, 1), (1, 0)])
            return v.astype(F32) + got.astype(F32)

        caches = write((k_out, v_out), kv_pair[1], 2, 0, 2, 4)
        attn_sum = add_over_y(attn)
        x_mid = (x_in.astype(F32) + attn_sum).astype(BF16)

        x_mid32 = x_mid.astype(F32)
        sq_mid = jnp.sum(x_mid32 * x_mid32, axis=1)
        local_scale = lax.rsqrt(sq_mid / width + EPS)
        h_local = (x_mid32 * local_scale[:, None] * g_ffn.astype(F32)).astype(BF16)
        r_part = lax.dot_general(w_router, h_local, (((0,), (1,)), ((), ())), preferred_element_type=F32)
        got = shared(jnp.concatenate([r_part, sq_mid[None, :]], axis=0), 1)
        sq_each = got[:, experts]
        full_scale = lax.rsqrt(jnp.sum(sq_each, axis=0) / width_full + EPS)
        logits = jnp.sum(got[:, :experts] * (full_scale[None, :] / lax.rsqrt(sq_each / width + EPS))[:, None, :], axis=0)
        h2 = (x_mid32 * full_scale[:, None] * g_ffn.astype(F32)).astype(BF16)
        eid = jnp.arange(experts)[:, None]
        pair = jnp.stack([jnp.sum(jnp.where(choice[None, :] == eid, logits, 0.0), axis=0) for choice in (choice_a, choice_b)])
        gates = jax.nn.softmax(pair, axis=0)
        n_pair = 2 * n_tok
        row_id = jnp.arange(n_pair)[:, None]
        at_a, at_b = pos_a[None, :] == row_id, pos_b[None, :] == row_id
        coef = jnp.sum(jnp.where(at_a, gates[0][None, :], 0.0) + jnp.where(at_b, gates[1][None, :], 0.0), axis=1, keepdims=True)
        sorted_h = jnp.dot((at_a | at_b).astype(BF16), h2, preferred_element_type=F32).astype(BF16)

        per_quarter = (ff + x_count * BLOCK - 1) // (x_count * BLOCK)
        first_blocks, last_blocks = list(range(per_quarter - 1)), [per_quarter - 1]
        w_down_t = w_down.transpose(0, 2, 1)

        def up(blocks):
            keep, send = up_experts(rel, offsets, sorted_h, w_act, w_lin, blocks, per_quarter)
            got = over_core(send)
            mine = (keep[0].astype(F32) + got[0].astype(F32)).astype(BF16)
            return mine, (keep[1].astype(F32) + got[1].astype(F32)).astype(BF16)

        def activate(mine, got):
            act, lin = (v for v in (mine.astype(F32) + got.astype(F32)).astype(BF16).astype(F32))
            unit = (coef * jax.nn.silu(act) * lin).astype(BF16)
            near = over_chip(unit)
            return unit, near, over_core(jnp.stack([unit, near]))

        def down(unit, before, blocks, last):
            return down_experts(rel, offsets, *unit, w_down_t, before, pos_a[:, None], pos_b[:, None], blocks, per_quarter, last)

        mine0, next0 = up(first_blocks)
        got0 = over_chip(next0)
        mine1, next1 = up(last_blocks)
        got1 = over_chip(next1)
        unit0 = activate(mine0, got0)
        caches = write(caches, kv_far[0], 1, 0, 1, 8)
        caches = write(caches, kv_far[1], 3, 0, 1, 8)
        unit1 = activate(mine1, got1)
        moe = down(unit0, None, first_blocks, False)
        moe = down(unit1, moe, last_blocks, True)
        k_out, v_out = write(caches, kv_pair[1], 2, 1, 2, 4)
        moe_sum = add_over_y(moe)
        out = (x_mid32 + moe_sum).astype(BF16)
        out = jnp.moveaxis(out.reshape(x_count, steps, per_q, width)[back], 0, 1).reshape(steps, n_batch, width)

        def to_cache(v):
            return v.reshape(n_batch, heads, head, -1).transpose(0, 3, 1, 2)

        return out, to_cache(k_out), to_cache(v_out)

    return jax.shard_map(layer_steps, mesh=mesh, in_specs=in_specs, out_specs=out_specs, check_vma=False)
```

```python
import jax
import jax.numpy as jnp
from jax import lax
from jax.experimental import pallas as pl
from jax.experimental.pallas import tpu as pltpu
from jax.sharding import PartitionSpec as P

EPS = 1e-5
ROPE_BASE = 1.0e6
LANES = 128
GROUP = 8
SLOTS = 4
TILE = 128
BLOCK = 256
ORDER = (0, 2, 1, 3)
VMEM_BYTES = 60 * 1024 * 1024
CORE_PERM = [(0, 1), (1, 0), (2, 3), (3, 2)]
CHIP_PERM = [(0, 2), (2, 0), (1, 3), (3, 1)]
F32 = jnp.float32
BF16 = jnp.bfloat16


def params(**kw):
    return pltpu.CompilerParams(vmem_limit_bytes=VMEM_BYTES, **kw)


def gather_rows(where, tokens, emb_table, n_tok, per_q, x_count):
    steps, n_batch = tokens.shape
    vocab, width = emb_table.shape
    last_tile = vocab // LANES - 1
    tail_at = (last_tile + 1) * LANES
    block_rows = steps * per_q
    n_block = n_tok // block_rows
    n_groups = n_tok // GROUP
    per_chunk = LANES // GROUP
    n_chunks = (n_tok + LANES - 1) // LANES

    def kernel(where_s, tok_s, tail_ref, emb_ref, out_ref, sq_ref, buf, acc, mine_s, sems):
        for k in range(n_block):
            quarter = lax.bitwise_xor(where_s[0], ORDER[k])
            for y in range(1, x_count // n_block):
                quarter = jnp.where(where_s[1] == y, lax.bitwise_xor(where_s[0], ORDER[y * n_block + k]), quarter)
            for t in range(steps):
                def note(bl, carry, k=k, t=t, quarter=quarter):
                    mine_s[k * block_rows + t * per_q + bl] = tok_s[t * n_batch + quarter * per_q + bl]
                    return carry

                lax.fori_loop(0, per_q, note, 0)

        def copy(g, i, tail=False):
            tile = jnp.minimum(mine_s[g * GROUP + i] // LANES, last_tile)
            slot = lax.rem(g, SLOTS)
            return pltpu.make_async_copy(
                tail_ref if tail else emb_ref.at[:, pl.ds(pl.multiple_of(tile * LANES, LANES), LANES)],
                buf.at[slot, :, pl.ds(i * LANES, LANES)], sems.at[slot, i])

        def start(g):
            for i in range(GROUP):
                in_tail = mine_s[g * GROUP + i] >= tail_at

                @pl.when(in_tail)
                def _():
                    copy(g, i, True).start()

                @pl.when(jnp.logical_not(in_tail))
                def _():
                    copy(g, i).start()

        for g in range(SLOTS - 1):
            start(g)
        lane_id = lax.broadcasted_iota(jnp.int32, (LANES, LANES), 0)
        col_id = lax.broadcasted_iota(jnp.int32, (LANES, LANES), 1)

        def step(g, carry):
            @pl.when(g + SLOTS - 1 < n_groups)
            def _():
                start(g + SLOTS - 1)

            for i in range(GROUP):
                copy(g, i).wait()
            slot = lax.rem(g, SLOTS)
            chunk = g // per_chunk
            base = lax.rem(g, per_chunk) * GROUP
            picks = []
            for i in range(GROUP):
                lane = lax.rem(mine_s[g * GROUP + i], LANES)
                picks.append(((lane_id == lane) & (col_id == base + i)).astype(F32).astype(BF16))
            pick = jnp.concatenate(picks, axis=0)
            for m in range(2):
                ds = pl.ds(m * (width // 2), width // 2)
                part = jnp.dot(buf[slot, ds, :], pick, preferred_element_type=F32)
                acc[chunk, ds, :] = jnp.where(base == 0, part, acc[chunk, ds, :] + part)
            return carry

        lax.fori_loop(0, n_groups, step, 0)
        for c in range(n_chunks):
            size = min(LANES, n_tok - c * LANES)
            rows = jnp.transpose(acc[c])[:size]
            out_ref[pl.ds(c * LANES, size), :] = rows.astype(BF16)
            sq_ref[pl.ds(c * LANES, size), :] = jnp.sum(rows * rows, axis=1, keepdims=True)

    return pl.pallas_call(
        kernel,
        out_shape=(jax.ShapeDtypeStruct((n_tok, width), BF16), jax.ShapeDtypeStruct((n_tok, 1), F32)),
        grid_spec=pltpu.PrefetchScalarGridSpec(
            num_scalar_prefetch=2, grid=(),
            in_specs=[pl.BlockSpec(memory_space=pl.ANY)] * 2,
            out_specs=[pl.BlockSpec(memory_space=pltpu.VMEM)] * 2,
            scratch_shapes=[pltpu.VMEM((SLOTS, width, GROUP * LANES), BF16), pltpu.VMEM((n_chunks, width, LANES), F32), pltpu.SMEM((n_tok,), jnp.int32), pltpu.SemaphoreType.DMA((SLOTS, GROUP))]),
        compiler_params=params(),
        cost_estimate=pl.CostEstimate(flops=2 * n_tok * width * LANES * LANES, bytes_accessed=n_tok * width * LANES * 2, transcendentals=0),
        name="gather_rows",
    )(where, tokens.reshape(-1), jnp.pad(emb_table[tail_at:].T, ((0, 0), (0, LANES - (vocab - tail_at)))), emb_table.T)


def column_scratch(rows_ref, out_ref):
    rows = rows_ref[...].astype(F32)
    pad = jnp.zeros((LANES - rows.shape[0], rows.shape[1]), F32)
    out_ref[...] = jnp.transpose(jnp.concatenate([rows, pad], axis=0)).astype(BF16)


def slot_masks(pos, row_local, per_q, steps, slots):
    col = lax.broadcasted_iota(jnp.int32, (LANES, slots), 0)
    slot = lax.broadcasted_iota(jnp.int32, (LANES, slots), 1)
    t = col // per_q
    pick = ((lax.rem(col, per_q) == row_local) & (slot == pos + t) & (t < steps)).astype(F32).astype(BF16)
    lane = lax.broadcasted_iota(jnp.int32, (16, slots), 1)
    keep = ((lane < pos) | (lane >= pos + steps)).astype(F32).astype(BF16)
    return pick, keep[:1]


def put_pair(blocks, columns, picks, keeps):
    slots = blocks[0].shape[1]
    new = jnp.dot(columns, jnp.concatenate(picks, axis=1), preferred_element_type=F32).astype(BF16)
    return [b * k + new[:, i * slots:(i + 1) * slots] for i, (b, k) in enumerate(zip(blocks, keeps))]


def cache_specs(k_cache, n_grid, step_b, skip=0):
    _, kv_width, slots = k_cache.shape
    return pl.BlockSpec((step_b, kv_width, slots), lambda g, qi, ln: (qi[0] * n_grid + skip + g, 0, 0))


def attend_part(quarter, lengths, q_rows, k_rows, v_rows, k_cache, v_cache, caches, heads, steps, part, n_parts):
    _, kv_width, slots = k_cache.shape
    per_q = q_rows.shape[0] // steps
    head = kv_width // heads
    h_pad = (heads + 7) // 8 * 8
    step_b = 4
    n_grid = per_q // step_b

    def kernel(qi, len_s, q_ref, kr_ref, vr_ref, kc_ref, vc_ref, *refs):
        o_ref, ko_ref, vo_ref, k_cols, v_cols = refs[-5:]
        g = pl.program_id(0)

        @pl.when(g == 0)
        def _():
            column_scratch(kr_ref, k_cols)
            column_scratch(vr_ref, v_cols)

        row_h = lax.broadcasted_iota(jnp.int32, (h_pad, kv_width), 0)
        col_h = lax.broadcasted_iota(jnp.int32, (h_pad, kv_width), 1) // head
        diag = row_h == col_h
        srow_t = lax.broadcasted_iota(jnp.int32, (steps * h_pad, slots), 0) // h_pad
        scol = lax.broadcasted_iota(jnp.int32, (steps * h_pad, slots), 1)
        bls = [g * step_b + i for i in range(step_b)]
        poss = [len_s[(qi[0] * n_parts + part) * per_q + bl] for bl in bls]
        picks, keeps = zip(*[slot_masks(pos, bl, per_q, steps, slots) for pos, bl in zip(poss, bls)])
        for i in range(0, step_b, 2):
            for src, cols, dst in ((kc_ref, k_cols, ko_ref), (vc_ref, v_cols, vo_ref)):
                for j, blk in enumerate(put_pair([src[i], src[i + 1]], cols[...], picks[i:i + 2], keeps[i:i + 2])):
                    dst[i + j] = blk
        scores, oks = [], []
        for i, (pos, bl) in enumerate(zip(poss, bls)):
            wide = jnp.concatenate([jnp.where(diag, q_ref[pl.ds(t * per_q + bl, 1), :], 0.0) for t in range(steps)], axis=0).astype(BF16)
            scores.append(jnp.dot(wide, ko_ref[i], preferred_element_type=F32) * head ** -0.5)
            oks.append((scol <= pos + srow_t).astype(F32))
        ok = jnp.concatenate(oks, axis=0) > 0.5
        s = jnp.where(ok, jnp.concatenate(scores, axis=0), -1.0e30)
        e = jnp.where(ok, jnp.exp(s - jnp.max(s, axis=1, keepdims=True)), 0.0)
        scale = 1.0 / jnp.sum(e, axis=1, keepdims=True)
        e = e.astype(BF16)
        n_row = steps * h_pad
        for i, bl in enumerate(bls):
            mine = slice(i * n_row, (i + 1) * n_row)
            mix = lax.dot_general(e[mine], vo_ref[i], (((1,), (1,)), ((), ())), preferred_element_type=F32) * scale[mine]
            for t in range(steps):
                piece = jnp.where(diag, mix[t * h_pad:(t + 1) * h_pad], 0.0)
                o_ref[pl.ds(t * per_q + bl, 1), :] = jnp.sum(piece, axis=0, keepdims=True)

    cache_in = cache_specs(k_cache, n_grid * n_parts, step_b, part * n_grid)
    anyspec = [pl.BlockSpec(memory_space=pl.ANY)] * len(caches)
    whole = lambda a: pl.BlockSpec(a.shape, lambda g, qi, ln: (0, 0))
    return pl.pallas_call(
        kernel,
        out_shape=(jax.ShapeDtypeStruct(q_rows.shape, F32), jax.ShapeDtypeStruct(k_cache.shape, BF16), jax.ShapeDtypeStruct(v_cache.shape, BF16)),
        grid_spec=pltpu.PrefetchScalarGridSpec(
            num_scalar_prefetch=2, grid=(n_grid,),
            in_specs=[whole(q_rows), whole(k_rows), whole(v_rows), cache_in, cache_in] + anyspec,
            out_specs=[pl.BlockSpec(q_rows.shape, lambda g, qi, ln: (0, 0)), cache_in, cache_in],
            scratch_shapes=[pltpu.VMEM((kv_width, LANES), BF16)] * 2),
        input_output_aliases={7: 1, 8: 2} if caches else {},
        compiler_params=params(),
        cost_estimate=pl.CostEstimate(flops=4 * per_q * kv_width * LANES * LANES, bytes_accessed=8 * per_q * kv_width * slots, transcendentals=0),
        name="attend_part",
    )(quarter, lengths, q_rows, k_rows, v_rows, k_cache, v_cache, *caches)


def copy_part(quarter, lengths, k_rows, v_rows, k_cache, v_cache, k_out, v_out, steps, part, n_parts, step_b):
    _, kv_width, slots = k_cache.shape
    per_q = k_rows.shape[0] // steps
    n_all = per_q // step_b
    n_grid = n_all // n_parts
    skip = part * n_grid

    def kernel(qi, len_s, kr_ref, vr_ref, kc_ref, vc_ref, ka_ref, va_ref, ko_ref, vo_ref, k_cols, v_cols):
        g = pl.program_id(0)

        @pl.when(g == 0)
        def _():
            column_scratch(kr_ref, k_cols)
            column_scratch(vr_ref, v_cols)

        for i in range(0, step_b, 2):
            bls = [(g + skip) * step_b + i + j for j in range(2)]
            poss = [len_s[qi[0] * per_q + bl] for bl in bls]
            picks, keeps = zip(*[slot_masks(pos, bl, per_q, steps, slots) for pos, bl in zip(poss, bls)])
            for src, cols, dst in ((kc_ref, k_cols, ko_ref), (vc_ref, v_cols, vo_ref)):
                for j, blk in enumerate(put_pair([src[i], src[i + 1]], cols[...], picks, keeps)):
                    dst[i + j] = blk

    cache_in = cache_specs(k_cache, n_all, step_b, skip)
    whole = lambda a: pl.BlockSpec(a.shape, lambda g, qi, ln: (0, 0))
    anyspec = pl.BlockSpec(memory_space=pl.ANY)
    return pl.pallas_call(
        kernel,
        out_shape=(jax.ShapeDtypeStruct(k_cache.shape, BF16), jax.ShapeDtypeStruct(v_cache.shape, BF16)),
        grid_spec=pltpu.PrefetchScalarGridSpec(
            num_scalar_prefetch=2, grid=(n_grid,),
            in_specs=[whole(k_rows), whole(v_rows), cache_in, cache_in, anyspec, anyspec],
            out_specs=[cache_in, cache_in],
            scratch_shapes=[pltpu.VMEM((kv_width, LANES), BF16)] * 2),
        input_output_aliases={6: 0, 7: 1},
        compiler_params=params(),
        cost_estimate=pl.CostEstimate(flops=4 * per_q // n_parts * kv_width * LANES * LANES, bytes_accessed=12 * per_q // n_parts * kv_width * slots, transcendentals=0),
        name="copy_part",
    )(quarter, lengths, k_rows, v_rows, k_cache, v_cache, k_out, v_out)


def expert_tiles(off_s, e, n_rows, body):
    lo, hi = off_s[e], off_s[e + 1]
    first = lo // 16 * 16
    n_tiles = jnp.where(hi > lo, (hi - first + TILE - 1) // TILE, 0)

    def step(i, carry):
        start = first + i * TILE
        at = pl.multiple_of(jnp.minimum(start, n_rows - TILE), 16)
        row = at + lax.broadcasted_iota(jnp.int32, (TILE, 1), 0)
        body(pl.ds(at, TILE), (row >= jnp.maximum(lo, start)) & (row < hi))
        return carry

    lax.fori_loop(0, n_tiles, step, 0)


def weight_specs(parts, per_quarter, blocks, depth):
    def spec(i, b):
        return pl.BlockSpec((1, depth, BLOCK), lambda e, rel, off: (e, 0, rel[i] * per_quarter + b))

    return [spec(i, b) for i in range(parts) for b in blocks]


def up_experts(rel, offsets, rows, w_act, w_lin, blocks, per_quarter):
    n_rows, depth = rows.shape
    experts, _, ff = w_act.shape
    parts, nb = rel.shape[0], len(blocks)
    n_w = parts * nb
    ragged = [b for b in blocks if ((parts - 1) * per_quarter + b + 1) * BLOCK > ff]

    def kernel(rel_s, off_s, x_ref, *refs):
        a_refs, l_refs, (keep_ref, send_ref) = refs[:n_w], refs[n_w:2 * n_w], refs[2 * n_w:]
        e = pl.program_id(0)
        lane = lax.broadcasted_iota(jnp.int32, (1, BLOCK), 1)

        def body(ds, mine):
            x = x_ref[ds, :]
            for i in range(parts):
                for n, b in enumerate(blocks):
                    ok = mine & (lane + (rel_s[i] * per_quarter + b) * BLOCK < ff) if b in ragged else mine
                    for k, w_refs in enumerate((a_refs, l_refs)):
                        out_ref = (keep_ref if i < 2 else send_ref).at[i % 2, k]
                        cols = pl.ds(n * BLOCK, BLOCK)
                        y = jnp.dot(x, w_refs[i * nb + n][0], preferred_element_type=F32)
                        out_ref[ds, cols] = jnp.where(ok, y, out_ref[ds, cols].astype(F32)).astype(BF16)

        if any(b in ragged for b in blocks):
            @pl.when(e == 0)
            def _():
                keep_ref[...] = jnp.zeros_like(keep_ref)
                send_ref[...] = jnp.zeros_like(send_ref)
        expert_tiles(off_s, e, n_rows, body)

    shape = (2, 2, n_rows, nb * BLOCK)
    out = pl.BlockSpec(shape, lambda e, rel, off: (0, 0, 0, 0))
    cols = n_w * BLOCK
    return pl.pallas_call(
        kernel,
        out_shape=(jax.ShapeDtypeStruct(shape, BF16),) * 2,
        grid_spec=pltpu.PrefetchScalarGridSpec(
            num_scalar_prefetch=2, grid=(experts,),
            in_specs=[pl.BlockSpec(rows.shape, lambda e, rel, off: (0, 0))] + weight_specs(parts, per_quarter, blocks, depth) * 2,
            out_specs=[out, out]),
        compiler_params=params(),
        cost_estimate=pl.CostEstimate(flops=8 * TILE * experts * depth * cols, bytes_accessed=6 * experts * depth * cols, transcendentals=0),
        name="up_experts",
    )(rel, offsets, rows, *[w_act] * n_w, *[w_lin] * n_w)


def down_experts(rel, offsets, own, near, far, w_down_t, before, pos_a, pos_b, blocks, per_quarter, last):
    n_rows = own.shape[0]
    experts, width, ff = w_down_t.shape
    n_tok = pos_a.shape[0]
    parts, nb = rel.shape[0], len(blocks)
    n_w = parts * nb
    edge = ff - (ff - 1) // BLOCK * BLOCK
    has_edge = per_quarter - 1 in blocks

    def kernel(rel_s, off_s, own_ref, near_ref, far_ref, *refs):
        w_refs, refs = refs[:n_w], refs[n_w:]
        if before is not None:
            before_ref, refs = refs[0], refs[1:]
        if last:
            pa_ref, pb_ref, out_ref, acc = refs
        else:
            acc, = refs
        e = pl.program_id(0)

        @pl.when(e == 0)
        def _():
            acc[...] = jnp.zeros_like(acc) if before is None else before_ref[...]

        def body(ds, mine):
            def run(edge_part):
                total = acc[ds, :]
                for i in range(parts):
                    for n, b in enumerate(blocks):
                        cut = edge if i == edge_part and b == per_quarter - 1 else BLOCK
                        cols = pl.ds(n * BLOCK, cut)
                        u = (own_ref[ds, cols], near_ref[ds, cols], far_ref[0, ds, cols], far_ref[1, ds, cols])[i]
                        w = w_refs[i * nb + n][0, :, :cut]
                        total = total + lax.dot_general(u, w, (((1,), (1,)), ((), ())), preferred_element_type=F32)
                acc[ds, :] = jnp.where(mine, total, acc[ds, :])

            if has_edge:
                for i in range(parts):
                    @pl.when(rel_s[i] == parts - 1)
                    def _(i=i):
                        run(i)
            else:
                run(None)

        expert_tiles(off_s, e, n_rows, body)

        if last:
            @pl.when(e == experts - 1)
            def _():
                col = lax.broadcasted_iota(jnp.int32, (n_tok, n_rows), 1)
                pick = ((col == pa_ref[...]) | (col == pb_ref[...])).astype(F32).astype(BF16)
                y = acc[...]
                high = y.astype(BF16)
                low = (y - high.astype(F32)).astype(BF16)
                out_ref[...] = (jnp.dot(pick, high, preferred_element_type=F32) + jnp.dot(pick, low, preferred_element_type=F32)).astype(BF16)

    whole = lambda a: pl.BlockSpec(a.shape, lambda e, rel, off: (0,) * a.ndim)
    extra = ([] if before is None else [before]) + ([pos_a, pos_b] if last else [])
    acc_shape = (n_rows, width)
    if last:
        out_shape, scratch = jax.ShapeDtypeStruct((n_tok, width), BF16), [pltpu.VMEM(acc_shape, F32)]
    else:
        out_shape, scratch = jax.ShapeDtypeStruct(acc_shape, F32), []
    cols = n_w * BLOCK
    return pl.pallas_call(
        kernel,
        out_shape=out_shape,
        grid_spec=pltpu.PrefetchScalarGridSpec(
            num_scalar_prefetch=2, grid=(experts,),
            in_specs=[whole(own), whole(near), whole(far)] + weight_specs(parts, per_quarter, blocks, width) + [whole(a) for a in extra],
            out_specs=pl.BlockSpec(out_shape.shape, lambda e, rel, off: (0, 0)),
            scratch_shapes=scratch),
        compiler_params=params(),
        cost_estimate=pl.CostEstimate(flops=4 * TILE * experts * cols * width, bytes_accessed=4 * experts * cols * width, transcendentals=0),
        name="down_experts",
    )(rel, offsets, own, near, far, *[w_down_t] * n_w, *extra)


def share_rows(rows, sums):
    n_x, n_y = 4, 2
    peers = [(d, e) for d in range(n_x) for e in range(n_y) if d or e]

    def kernel(rows_ref, sums_ref, rows_out, sums_out, send_sems, recv_sems):
        xi, yi = lax.axis_index('x'), lax.axis_index('y')

        def peer(d, e):
            return {'x': lax.bitwise_xor(xi, d), 'y': lax.bitwise_xor(yi, e)}

        barrier = pltpu.get_barrier_semaphore()
        for d, e in peers:
            pl.semaphore_signal(barrier, inc=1, device_id=peer(d, e), device_id_type=pl.DeviceIdType.MESH)
        pl.semaphore_wait(barrier, len(peers))
        copies = [pltpu.make_async_remote_copy(
            src_ref=rows_ref, dst_ref=rows_out.at[yi], send_sem=send_sems.at[0], recv_sem=recv_sems.at[0],
            device_id=peer(0, 1), device_id_type=pl.DeviceIdType.MESH)]
        copies += [pltpu.make_async_remote_copy(
            src_ref=sums_ref, dst_ref=sums_out.at[d, yi], send_sem=send_sems.at[k + 1], recv_sem=recv_sems.at[k + 1],
            device_id=peer(d, e), device_id_type=pl.DeviceIdType.MESH) for k, (d, e) in enumerate(peers)]
        for c in copies:
            c.start()
        rows_out[yi] = rows_ref[...]
        sums_out[0, yi] = sums_ref[...]
        for c in copies:
            c.wait()

    return pl.pallas_call(
        kernel,
        out_shape=(jax.ShapeDtypeStruct((n_y,) + rows.shape, rows.dtype), jax.ShapeDtypeStruct((n_x, n_y) + sums.shape, sums.dtype)),
        in_specs=[pl.BlockSpec(memory_space=pltpu.VMEM)] * 2,
        out_specs=[pl.BlockSpec(memory_space=pltpu.VMEM)] * 2,
        scratch_shapes=[pltpu.SemaphoreType.DMA((len(peers) + 1,))] * 2,
        compiler_params=pltpu.CompilerParams(collective_id=0, has_side_effects=True),
        cost_estimate=pl.CostEstimate(flops=0, bytes_accessed=16_000_000, transcendentals=0),
        name="share_rows",
    )(rows, sums)


def share_small(values, call_id):
    n_dev = 4

    def kernel(v_ref, out_ref, send_sems, recv_sems):
        xi = lax.axis_index('x')
        barrier = pltpu.get_barrier_semaphore()
        for d in range(1, n_dev):
            pl.semaphore_signal(barrier, inc=1, device_id={'x': lax.bitwise_xor(xi, d)}, device_id_type=pl.DeviceIdType.MESH)
        pl.semaphore_wait(barrier, n_dev - 1)
        copies = []
        for d in range(1, n_dev):
            copies.append(pltpu.make_async_remote_copy(
                src_ref=v_ref, dst_ref=out_ref.at[d], send_sem=send_sems.at[d - 1], recv_sem=recv_sems.at[d - 1],
                device_id={'x': lax.bitwise_xor(xi, d)}, device_id_type=pl.DeviceIdType.MESH))
            copies[-1].start()
        out_ref[0] = v_ref[...]
        for c in copies:
            c.wait()

    return pl.pallas_call(
        kernel,
        out_shape=jax.ShapeDtypeStruct((n_dev,) + values.shape, values.dtype),
        in_specs=[pl.BlockSpec(memory_space=pltpu.VMEM)],
        out_specs=pl.BlockSpec(memory_space=pltpu.VMEM),
        scratch_shapes=[pltpu.SemaphoreType.DMA((n_dev - 1,))] * 2,
        compiler_params=pltpu.CompilerParams(collective_id=call_id, has_side_effects=True),
        cost_estimate=pl.CostEstimate(flops=0, bytes_accessed=8_000_000, transcendentals=0),
        name="share_small",
    )(values)


def solution(mesh):
    x_count = mesh.shape['x']
    cache_spec = P('dp', None, 'y', None)
    in_specs = (P(None, 'dp'), P('dp'), P(None, 'dp', None), P(None, 'x'), cache_spec, cache_spec, P('x'), P('x', 'y'), P('x', 'y'), P('x', 'y'), P('y', 'x'), P('x'), P('x', None), P(None, 'x', 'y'), P(None, 'x', 'y'), P(None, 'y', 'x'))
    out_specs = (P(None, 'dp', 'x'), cache_spec, cache_spec)

    def over_core(v):
        return lax.ppermute(v, 'x', CORE_PERM)

    def over_chip(v):
        return lax.ppermute(v, 'x', CHIP_PERM)

    def layer_steps(tokens, lengths, choices, emb_table, k_cache, v_cache, g_attn, w_q, w_k, w_v, w_o, g_ffn, w_router, w_act, w_lin, w_down):
        steps, n_batch = tokens.shape
        heads, head = k_cache.shape[2], k_cache.shape[3]
        kv_width = heads * head
        width = emb_table.shape[1]
        width_full = width * x_count
        experts, _, ff = w_act.shape
        n_tok = steps * n_batch
        per_q = n_batch // x_count
        q_rows_n = steps * per_q
        n_group = 2
        g_rows = q_rows_n // n_group
        xi = lax.axis_index('x')
        order = jnp.array(ORDER, jnp.int32)
        rel = lax.bitwise_xor(order, xi)
        back = order[lax.bitwise_xor(jnp.arange(x_count, dtype=jnp.int32), xi)]

        def to_rel(a):
            a = a.reshape((steps, x_count, per_q) + a.shape[2:])
            return jnp.moveaxis(a, 1, 0)[rel].reshape((n_tok,) + a.shape[3:])

        def shared(v, call_id):
            r = v.shape[0]
            v = jnp.pad(v, ((0, -r % 8), (0, 0)))
            got = share_small(jnp.moveaxis(v.reshape(-1, x_count, q_rows_n), 1, 0), call_id)
            rows = [[got[d, ORDER[ORDER[i] ^ d], :r] for i in range(x_count)] for d in range(x_count)]
            return jnp.stack([jnp.concatenate(one, axis=1) for one in rows])

        yi = lax.axis_index('y')
        y_rows = n_tok // 2
        my_rows, my_sq = gather_rows(jnp.stack([xi, yi]), tokens, emb_table, y_rows, per_q, x_count)
        both_rows, each_sq = share_rows(my_rows, jnp.pad(my_sq.reshape(2, 1, q_rows_n), ((0, 0), (0, 7), (0, 0))))
        x_in = both_rows.reshape(n_tok, width)
        found = [[ORDER[ORDER[i] ^ d] for d in range(x_count)] for i in range(x_count)]
        total_sq = jnp.stack([sum(each_sq[d, j // 2, j % 2, 0] for d, j in enumerate(js)) for js in found]).reshape(n_tok, 1)
        h = (x_in.astype(F32) * lax.rsqrt(total_sq / width_full + EPS) * g_attn.astype(F32)).astype(BF16)
        part = jnp.concatenate([jnp.dot(h, w, preferred_element_type=F32) for w in (w_q, w_k, w_v)], axis=1).astype(BF16)

        choices, lengths_r, part = lax.optimization_barrier((choices, lengths, part))
        flat = choices.reshape(n_tok * 2)
        hot = (flat[:, None] == jnp.arange(experts)[None, :])
        lower = (lax.broadcasted_iota(jnp.int32, (2 * n_tok, 2 * n_tok), 0) > lax.broadcasted_iota(jnp.int32, (2 * n_tok, 2 * n_tok), 1)).astype(BF16)
        before = jnp.dot(lower, hot.astype(BF16), preferred_element_type=F32).astype(jnp.int32)
        counts = jnp.sum(hot.astype(jnp.int32), axis=0)
        first = jnp.sum(jnp.where(jnp.arange(experts)[:, None] > jnp.arange(experts)[None, :], counts[None, :], 0), axis=1)
        offsets = jnp.concatenate([first, jnp.full((1,), 2 * n_tok, jnp.int32)])
        place = jnp.sum(jnp.where(hot, before + first[None, :], 0), axis=1).reshape(steps, n_batch, 2)
        pos_a = to_rel(place[:, :, 0])
        pos_b = to_rel(place[:, :, 1])
        choice_a = to_rel(choices[:, :, 0])
        choice_b = to_rel(choices[:, :, 1])

        len_q = lax.dynamic_slice(lengths_r, (xi * per_q,), (per_q,))
        positions = (len_q[None, :] + jnp.arange(steps)[:, None]).reshape(q_rows_n).astype(F32)
        inv_freq = ROPE_BASE ** (-(jnp.arange(head // 2, dtype=F32) * 2.0 / head))
        angles = jnp.tile(positions[:, None] * inv_freq[None, :], (1, 2 * heads))
        cosine, sine = jnp.cos(angles), jnp.sin(angles)
        low_half = (jnp.arange(kv_width) % head < head // 2)[None, :]

        def rotate(v, cosine, sine):
            other = jnp.where(low_half, -jnp.roll(v, -(head // 2), axis=1), jnp.roll(v, head // 2, axis=1))
            return (v * cosine + other * sine).astype(BF16)

        def grouped(a):
            return a.reshape(a.shape[0] // per_q, n_group, per_q // n_group, -1)

        cosine, sine = grouped(cosine), grouped(sine)
        part = part.reshape(x_count, steps, n_group, per_q // n_group, -1)
        firsts = []
        for g in range(n_group):
            one = part[:, :, g].reshape(x_count, g_rows, -1)
            got = over_core(one[2:])
            mine, away = ((one[i].astype(F32) + got[i].astype(F32)).astype(BF16) for i in range(2))
            firsts.append((mine, over_chip(away)))
        k_view = k_cache.transpose(0, 2, 3, 1).reshape(n_batch, kv_width, -1)
        v_view = v_cache.transpose(0, 2, 3, 1).reshape(n_batch, kv_width, -1)
        caches, kv_groups, mixed_groups = (), [], []
        for g, (mine, got) in enumerate(firsts):
            proj = (mine.astype(F32) + got.astype(F32)).astype(BF16).astype(F32)
            cos_g, sin_g = cosine[:, g].reshape(g_rows, -1), sine[:, g].reshape(g_rows, -1)
            queries = rotate(proj[:, :kv_width], cos_g, sin_g).astype(F32)
            keys = rotate(proj[:, kv_width:2 * kv_width], cos_g, sin_g)
            vals = proj[:, 2 * kv_width:].astype(BF16)
            mixed, *caches = attend_part(xi[None], lengths, queries, keys, vals, k_view, v_view, caches, heads, steps, g, n_group)
            kv_groups.append(jnp.concatenate([keys, vals], axis=1).reshape(steps, per_q // n_group, -1))
            mixed = mixed.astype(BF16)
            mixed_groups.append(jnp.stack([mixed, over_chip(mixed)]))
        attn_groups = []
        for mixed2 in mixed_groups:
            mixed4 = jnp.concatenate([mixed2, over_core(mixed2)], axis=0).reshape(x_count * g_rows, -1)
            attn_groups.append(jnp.dot(mixed4, w_o, preferred_element_type=F32).astype(BF16))
        kv_new = jnp.stack(kv_groups, axis=1).reshape(q_rows_n, -1)

        kv_pair = jnp.stack([kv_new, over_chip(kv_new)])
        kv_far = over_core(kv_pair)

        def write(caches, rows, idx, part, n_parts, step_b):
            return copy_part(lax.bitwise_xor(xi, idx)[None], lengths, rows[:, :kv_width], rows[:, kv_width:], k_view, v_view, *caches, steps, part, n_parts, step_b)

        def add_over_y(v):
            got = lax.ppermute(v, 'y', [(0, 1), (1, 0)])
            return v.astype(F32) + got.astype(F32)

        attn_sum = jnp.stack([add_over_y(v).reshape(x_count, steps, per_q // n_group, width) for v in attn_groups], axis=2).reshape(n_tok, width)
        x_mid = (x_in.astype(F32) + attn_sum).astype(BF16)

        x_mid32 = x_mid.astype(F32)
        sq_mid = jnp.sum(x_mid32 * x_mid32, axis=1)
        local_scale = lax.rsqrt(sq_mid / width + EPS)
        h_local = (x_mid32 * local_scale[:, None] * g_ffn.astype(F32)).astype(BF16)
        r_part = lax.dot_general(w_router, h_local, (((0,), (1,)), ((), ())), preferred_element_type=F32)
        got = shared(jnp.concatenate([r_part, sq_mid[None, :]], axis=0), 1)
        sq_each = got[:, experts]
        full_scale = lax.rsqrt(jnp.sum(sq_each, axis=0) / width_full + EPS)
        logits = jnp.sum(got[:, :experts] * (full_scale[None, :] / lax.rsqrt(sq_each / width + EPS))[:, None, :], axis=0)
        h2 = (x_mid32 * full_scale[:, None] * g_ffn.astype(F32)).astype(BF16)
        eid = jnp.arange(experts)[:, None]
        pair = jnp.stack([jnp.sum(jnp.where(choice[None, :] == eid, logits, 0.0), axis=0) for choice in (choice_a, choice_b)])
        gates = jax.nn.softmax(pair, axis=0)
        n_pair = 2 * n_tok
        row_id = jnp.arange(n_pair)[:, None]
        at_a, at_b = pos_a[None, :] == row_id, pos_b[None, :] == row_id
        coef = jnp.sum(jnp.where(at_a, gates[0][None, :], 0.0) + jnp.where(at_b, gates[1][None, :], 0.0), axis=1, keepdims=True)
        sorted_h = jnp.dot((at_a | at_b).astype(BF16), h2, preferred_element_type=F32).astype(BF16)

        per_quarter = (ff + x_count * BLOCK - 1) // (x_count * BLOCK)
        first_blocks, last_blocks = list(range(per_quarter - 1)), [per_quarter - 1]
        w_down_t = w_down.transpose(0, 2, 1)

        def up(blocks):
            keep, send = up_experts(rel, offsets, sorted_h, w_act, w_lin, blocks, per_quarter)
            got = over_core(send)
            mine = (keep[0].astype(F32) + got[0].astype(F32)).astype(BF16)
            return mine, (keep[1].astype(F32) + got[1].astype(F32)).astype(BF16)

        def activate(mine, got):
            act, lin = (v for v in (mine.astype(F32) + got.astype(F32)).astype(BF16).astype(F32))
            unit = (coef * jax.nn.silu(act) * lin).astype(BF16)
            near = over_chip(unit)
            return unit, near, over_core(jnp.stack([unit, near]))

        def down(unit, before, blocks, last):
            return down_experts(rel, offsets, *unit, w_down_t, before, pos_a[:, None], pos_b[:, None], blocks, per_quarter, last)

        mine0, next0 = up(first_blocks)
        got0 = over_chip(next0)
        mine1, next1 = up(last_blocks)
        got1 = over_chip(next1)
        unit0 = activate(mine0, got0)
        caches = write(caches, kv_far[0], 1, 0, 1, 8)
        caches = write(caches, kv_far[1], 3, 0, 1, 8)
        caches = write(caches, kv_pair[1], 2, 0, 2, 4)
        unit1 = activate(mine1, got1)
        moe = down(unit0, None, first_blocks, False)
        moe = down(unit1, moe, last_blocks, True)
        k_out, v_out = write(caches, kv_pair[1], 2, 1, 2, 4)
        moe_sum = add_over_y(moe)
        out = (x_mid32 + moe_sum).astype(BF16)
        out = jnp.moveaxis(out.reshape(x_count, steps, per_q, width)[back], 0, 1).reshape(steps, n_batch, width)

        def to_cache(v):
            return v.reshape(n_batch, heads, head, -1).transpose(0, 3, 1, 2)

        return out, to_cache(k_out), to_cache(v_out)

    return jax.shard_map(layer_steps, mesh=mesh, in_specs=in_specs, out_specs=out_specs, check_vma=False)
```
